256 devices in a mesh: tm: 64 (over x, z, core), env: 4 (over y).
Axes of the slice: x: 4, y: 4, z: 8, core: 2. Of those that a mesh axis runs over, the one named last changes fastest.
Arguments:
- init_state: float32 [70, 1024], P(None, 'env'), may hold values from -6 to 6
- torque: float32 [256, 35, 1024], P('tm', None, 'env'), may hold values from -192 to 192
- contact: int32 [256, 1024], P('tm', 'env'), may hold values 0 or 1
- mass_inverse: float32 [128, 35, 35], P('tm'), may hold values from -0.014 to 1.5, as said below
- stiffness: float32 [35], replicated, may hold values from 10 to 100
- damping: float32 [35], replicated, may hold values from 0.5 to 5
- gravity: float32 [35], replicated, may hold values from 1 to 10
- contact_stiffness: float32 [35], replicated, may hold values from 20 to 100
- contact_damping: float32 [35], replicated, may hold values from 0.5 to 3
Outputs:
- final_states: float32 [128, 70, 1024], P('tm', None, 'env')
- corrections: float32 [3, 1024], P(None, 'env')
The draws below stay inside these ranges and needn't reach their ends.
Inputs may be any that keep to these rules, and one draw needn't show every extreme that they name: `mass_inverse`: each matrix is symmetric, and each diagonal entry exceeds the sum of the magnitudes of the other entries of its row.
All inputs are finite; a program needn't handle non-finite values. No bound on the sum of `contact` on one device may be relied on, other than what follows from the above.
Results may differ from the reference program's by a relative error of at most 0.00025.
Values sent between devices are 32-bit elements; how exact they have to be, the bound alone decides.
No kernel may reach another device: no remote copies, remote signals or barrier semaphores. Data moves between devices by JAX's collectives and lax.ppermute only.
A program may use at most 64 MiB of HBM per device.

```python
import math
import jax
import jax.numpy as jnp
from jax import lax

DOF = 35
STATE = 70
HS = 2
SUB = 32
ITERS = 3
SLICES = 128
STEPS = 256
ENV = 1024


def draw_mass_inverse(key, part):
    key_diag = jax.random.fold_in(key, 11)
    key_off = jax.random.fold_in(key, 12)
    diagonal = jax.random.uniform(key_diag, (SLICES, DOF), jnp.float32, 0.5, 1.5)
    raw = jnp.clip(0.008 * jax.random.normal(key_off, (SLICES, DOF, DOF), jnp.float32), -0.014, 0.014)
    upper = jnp.triu(raw, 1)
    return upper + jnp.swapaxes(upper, 1, 2) + diagonal[:, :, None] * jnp.eye(DOF, dtype=jnp.float32)


def touch_ends(values, own_key, low, largest):
    spot = [jax.random.randint(jax.random.fold_in(own_key, axis), (), 0, length) for axis, length in enumerate(values.shape)]
    widest = values.shape.index(max(values.shape))
    neighbour = spot[:widest] + [(spot[widest] + 1) % values.shape[widest]] + spot[widest + 1:]
    return values.at[tuple(spot)].set(low).at[tuple(neighbour)].set(largest)


def shard_levels(key, extent, cuts, low, largest):
    factor_of, own = 1.0, jax.random.fold_in(key, 6)
    for position, shards_of in cuts:
        draws = jnp.exp(jax.random.uniform(jax.random.fold_in(own, position), (shards_of,), jnp.float32, low / len(cuts), largest / len(cuts)))
        factor_of = factor_of * jnp.repeat(draws, extent[position] // shards_of).reshape([-1 if axis == position else 1 for axis in range(len(extent))])
    return factor_of


def gaussian(own_key, dims, deviation, most, shards=(), kind=jnp.bfloat16):
    array = jax.random.normal(own_key, dims, jnp.float32) * deviation
    if len(shards) > 0:
        array = shard_levels(own_key, dims, shards, -0.22, 0.18) * array
    return jnp.clip(array, min=-most, max=most).astype(kind)


def setup_inputs(seed: int = 0) -> dict:
    arg_keys = jax.random.split(jax.random.key(seed), 10)
    return {
        "init_state": gaussian(arg_keys[0], (STATE, ENV), 0.5, 6.0, ((1, 4),), jnp.float32),
        "torque": gaussian(arg_keys[1], (STEPS, DOF, ENV), 30.0, 192.0, ((0, 64), (2, 4)), jnp.float32),
        "contact": touch_ends((jax.random.randint(arg_keys[2], (STEPS, ENV), 0, 3) < 1).astype(jnp.int32), jax.random.fold_in(arg_keys[2], 1), 0, 1),
        "mass_inverse": draw_mass_inverse(jax.random.fold_in(arg_keys[9], 71), 0),
        "stiffness": jnp.clip(jnp.exp(jax.random.uniform(arg_keys[4], (DOF,), jnp.float32, math.log(10.0), math.log(100.0))), 10.0, 100.0),
        "damping": jnp.clip(jnp.exp(jax.random.uniform(arg_keys[5], (DOF,), jnp.float32, math.log(0.5), math.log(5.0))), 0.5, 5.0),
        "gravity": jnp.clip(jnp.exp(jax.random.uniform(arg_keys[6], (DOF,), jnp.float32, math.log(1.0), math.log(10.0))), 1.0, 10.0),
        "contact_stiffness": jnp.clip(jnp.exp(jax.random.uniform(arg_keys[7], (DOF,), jnp.float32, math.log(20.0), math.log(100.0))), 20.0, 100.0),
        "contact_damping": jnp.clip(jnp.exp(jax.random.uniform(arg_keys[8], (DOF,), jnp.float32, math.log(0.5), math.log(3.0))), 0.5, 3.0),
    }


step_length = 0.05

def exact_dot(left, right):
    return jnp.dot(left, right, precision=lax.Precision.HIGHEST, preferred_element_type=jnp.float32)

def coarse_one(state_now, torque_steps, mean_steps, inverse, params):
    stiffness, damping, gravity, contact_stiffness, contact_damping = params
    joint_pos = state_now[:DOF]
    joint_vel = state_now[DOF:]
    for step_pos in range(HS):
        spring = (stiffness + gravity + mean_steps[step_pos] * contact_stiffness)[:, None]
        friction = (damping + mean_steps[step_pos] * contact_damping)[:, None]
        force = torque_steps[step_pos] - spring * joint_pos - friction * joint_vel
        joint_vel = joint_vel + step_length * exact_dot(inverse, force)
        joint_pos = joint_pos + step_length * joint_vel
    return jnp.concatenate([joint_pos, joint_vel], axis=0)

def fine_one(state_now, torque_steps, contact_steps, inverse, params):
    stiffness, damping, gravity, contact_stiffness, contact_damping = params
    fine_dt = step_length / SUB
    joint_pair = (state_now[:DOF], state_now[DOF:])
    for step_pos in range(HS):
        torque_here = torque_steps[step_pos]
        contact_here = contact_steps[step_pos][None, :]

        def substep(counter, pair_now):
            joint_pos, joint_vel = pair_now
            force = torque_here - stiffness[:, None] * joint_pos - damping[:, None] * joint_vel - gravity[:, None] * jnp.sin(joint_pos) - contact_here * (contact_stiffness[:, None] * joint_pos + contact_damping[:, None] * joint_vel)
            joint_vel = joint_vel + fine_dt * exact_dot(inverse, force)
            joint_pos = joint_pos + fine_dt * joint_vel
            return (joint_pos, joint_vel)
        joint_pair = lax.fori_loop(0, SUB, substep, joint_pair)
    return jnp.concatenate([joint_pair[0], joint_pair[1]], axis=0)

def reference(init_state, torque, contact, mass_inverse, stiffness, damping, gravity, contact_stiffness, contact_damping):
    params = (stiffness, damping, gravity, contact_stiffness, contact_damping)
    torque_steps = torque.reshape(SLICES, HS, DOF, ENV)
    contact_steps = contact.astype(jnp.float32).reshape(SLICES, HS, ENV)
    mean_steps = lax.optimization_barrier(jnp.mean(contact_steps, axis=2))
    coarse_all = jax.vmap(coarse_one, in_axes=(0, 0, 0, 0, None))
    fine_all = jax.vmap(fine_one, in_axes=(0, 0, 0, 0, None))

    def chain(jumps):

        def advance(state_now, inputs):
            torque_here, mean_here, inverse, jump = inputs
            following = coarse_one(state_now, torque_here, mean_here, inverse, params) + jump
            return (following, following)
        unused, ends = lax.scan(advance, init_state, (torque_steps, mean_steps, mass_inverse, jumps))
        return ends
    ends = chain(jnp.zeros((SLICES, STATE, ENV), jnp.float32))
    records = []
    for iteration in range(ITERS):
        starts = jnp.concatenate([init_state[None], ends[:-1]], axis=0)
        jumps = fine_all(starts, torque_steps, contact_steps, mass_inverse, params) - coarse_all(starts, torque_steps, mean_steps, mass_inverse, params)
        new_ends = chain(jumps)
        records.append(lax.optimization_barrier(jnp.max(jnp.sqrt(lax.optimization_barrier(jnp.sum((new_ends - ends) ** 2, axis=1))), axis=0)))
        ends = new_ends
    return (ends, jnp.stack(records))
```

```python
import functools
import math

import jax
import jax.numpy as jnp
from jax import lax
from jax.experimental import pallas as pl
from jax.experimental.pallas import tpu as pltpu
from jax.sharding import Mesh
from jax.sharding import PartitionSpec as P

DOF = 35
PAD = 40
HS = 2
SUB = 32
ITERS = 3
GROUP = 4
BLOCKS = 4
CHIPS = 32
STEPS = GROUP * HS
LANES = 128
ENV = 1024
TM = ("x", "z", "c")
PEERS = ("y", "x", "z")

DT = 0.05
FINE = DT / SUB
TURN = 1.0 / (2.0 * math.pi)
SINE = (6.283182595389212, -16.20867027746649, 16.7609745050196, -9.530799181282873, 3.0583252710952205)

ROW_CONTACT = STEPS * PAD
ROW_COUNT = ROW_CONTACT + 8
ROW_INIT = ROW_COUNT + 8
ROW_MASS = 512
CHUNKS = 16
OUT_CHUNKS = 4
VMEM_LIMIT = 56 * 1024 * 1024

f32 = jnp.float32


def lane_index(rows):
    return lax.broadcasted_iota(jnp.int32, (rows, LANES), 1)


def block_transpose(parts):
    lane = lane_index(parts[0].shape[0])
    low = lane < 64
    even = ((lane >> 5) & 1) == 0
    a, b, c, d = parts
    a, c = jnp.where(low, a, pltpu.roll(c, 64, 1)), jnp.where(low, pltpu.roll(a, 64, 1), c)
    b, d = jnp.where(low, b, pltpu.roll(d, 64, 1)), jnp.where(low, pltpu.roll(b, 64, 1), d)
    a, b = jnp.where(even, a, pltpu.roll(b, 32, 1)), jnp.where(even, pltpu.roll(a, 96, 1), b)
    c, d = jnp.where(even, c, pltpu.roll(d, 32, 1)), jnp.where(even, pltpu.roll(c, 96, 1), d)
    return a, b, c, d


def block_spread(value):
    block = lane_index(value.shape[0]) >> 5
    turned = [value] + [pltpu.roll(value, 32 * m, 1) for m in (1, 2, 3)]
    return [
        jnp.where(
            block < 2,
            jnp.where(block == 0, turned[(0 - c) % 4], turned[(1 - c) % 4]),
            jnp.where(block == 2, turned[(2 - c) % 4], turned[(3 - c) % 4]),
        )
        for c in range(4)
    ]


def shifted(value, by):
    group = lane_index(value.shape[0]) & 31
    return jnp.where(group >= by, pltpu.roll(value, by, 1), 0.0)


def pack_kernel(torque, contact, counts, init, mass, out, rows):
    rows[...] = jnp.zeros_like(rows)
    for t in range(STEPS):
        rows[t * PAD : t * PAD + DOF, :] = torque[t]
    rows[ROW_CONTACT : ROW_CONTACT + 8, :] = contact[...]
    rows[ROW_COUNT : ROW_COUNT + 8, :] = jnp.broadcast_to(counts[...], (8, LANES))
    rows[ROW_INIT : ROW_INIT + DOF, :] = init[:DOF, :]
    rows[ROW_INIT + PAD : ROW_INIT + PAD + DOF, :] = init[DOF:, :]
    for c in range(4):
        out[:, c, :] = rows[c * LANES : (c + 1) * LANES, :].T
    for c in range(4, CHUNKS):
        out[:, c, :] = jnp.broadcast_to(mass[c - 4 : c - 3, :], (LANES, LANES))


def state_row(k):
    return k if k < DOF else k + PAD - DOF


def main_kernel(
    recv, par, out, rows, mb, ma, wide, cols, tau_b, stiff_b, damp_b, spring, fric, start, end, shift, diff, pos, vel, force, vec, corr
):
    for c in range(CHUNKS - 1):
        rows[c * LANES : (c + 1) * LANES, :] = recv[:, c, :].T

    def param(i):
        return jnp.broadcast_to(par[:, i : i + 1], (PAD, LANES))

    stiffness, damping, gravity, contact_stiffness, contact_damping = (param(i) for i in range(5))

    mb[...] = jnp.zeros_like(mb)
    ma[...] = jnp.zeros_like(ma)

    def place_mass(k, carry):
        part = rows[pl.ds(pl.multiple_of(ROW_MASS + k * PAD, 8), PAD), :]
        mb[k] = part
        for b, spread in enumerate(block_spread(part)):
            ma[b, k] = spread
        return carry

    lax.fori_loop(0, DOF, place_mass, 0)

    count = rows[ROW_COUNT : ROW_COUNT + 8, :]
    total = count + pltpu.roll(count, 32, 1) + pltpu.roll(count, 64, 1) + pltpu.roll(count, 96, 1)
    mean = total / ENV
    for t in range(STEPS):
        here = mean[t : t + 1, :]
        spring[t] = (stiffness + gravity + here * contact_stiffness) * (FINE * DT)
        fric[t] = (damping + here * contact_damping) * DT

    for j in range(HS):
        turned = block_transpose([rows[(2 * b + j) * PAD : (2 * b + j + 1) * PAD, :] for b in range(GROUP)])
        touch = block_transpose(
            [rows[ROW_CONTACT + 2 * b + j : ROW_CONTACT + 2 * b + j + 1, :] for b in range(GROUP)]
        )
        for e in range(BLOCKS):
            tau_b[j, e] = turned[e] * (FINE * FINE * TURN)
            stiff_b[j, e] = (stiffness + touch[e] * contact_stiffness) * (FINE * FINE)
            damp_b[j, e] = (damping + touch[e] * contact_damping) * FINE

    grav = gravity * (FINE * FINE * TURN)

    def half_step(b, t, q, w, driven):
        pull = spring[t] * q + fric[t] * w
        if driven:
            at = t * PAD if isinstance(t, int) else pl.multiple_of(t * PAD, 8)
            pull = rows[pl.ds(at, PAD), :] * (FINE * DT * TURN) - pull
        else:
            pull = -pull
        vec[0:PAD, :] = pull
        for k in range(DOF):
            w = w + ma[b, k] * vec[k : k + 1, :]
        return q + float(SUB) * w, w

    def slice_step(b, q, w, driven):
        q, w = half_step(b, 2 * b, q, w, driven)
        return half_step(b, 2 * b + 1, q, w, driven)

    def apply_wide(level, value):
        vec[...] = value
        total = None
        for k in range(2 * DOF):
            term = wide[level, k] * vec[state_row(k) : state_row(k) + 1, :]
            total = term if total is None else total + term
        return total

    row80 = lax.broadcasted_iota(jnp.int32, (2 * PAD, LANES), 0)
    col_block = lane_index(2 * PAD) >> 5

    def spread_columns(level, cg, value):
        for c, spread in enumerate(block_spread(value)):
            wide[level, 4 * cg + c] = spread

    def first_columns(cg, carry):
        col = 4 * cg + col_block
        col = jnp.where(col < DOF, col, col + (PAD - DOF))
        unit = jnp.where(row80 == col, 1.0, 0.0)

        def one(b, qw):
            return slice_step(b, qw[0], qw[1], False)

        q, w = lax.fori_loop(0, GROUP, one, (unit[:PAD], unit[PAD:]))
        value = jnp.concatenate([q, w], axis=0)
        cols[cg] = value
        spread_columns(0, cg, value)
        return carry

    lax.fori_loop(0, 18, first_columns, 0)
    for level, by in ((1, 1), (2, 2)):

        def more_columns(cg, carry, level=level, by=by):
            value = apply_wide(level - 1, shifted(cols[cg], by))
            cols[cg] = value
            spread_columns(level, cg, value)
            return carry

        lax.fori_loop(0, 18, more_columns, 0)

    def scan_groups(value):
        value = value + apply_wide(0, shifted(value, 1))
        value = value + apply_wide(1, shifted(value, 2))
        diff[0] = value

        def more(i, running):
            return diff[0] + apply_wide(2, shifted(running, 4))

        return lax.fori_loop(0, 7, more, value)

    first = (lane_index(2 * PAD) & 31) == 0
    init = jnp.where(first, rows[ROW_INIT : ROW_INIT + 2 * PAD, :], 0.0)
    init = jnp.concatenate([init[:PAD] * TURN, init[PAD:] * (FINE * TURN)], axis=0)

    def driven_slice(b, qw):
        return slice_step(b, qw[0], qw[1], True)

    q, w = lax.fori_loop(0, GROUP, driven_slice, (init[:PAD], init[PAD:]))
    ends = scan_groups(jnp.concatenate([q, w], axis=0))
    entry = jnp.where(first, init, shifted(ends, 1))

    def driven_keep(b, qw):
        start[b] = jnp.concatenate(qw, axis=0)
        qw = slice_step(b, qw[0], qw[1], True)
        end[b] = jnp.concatenate(qw, axis=0)
        return qw

    lax.fori_loop(0, GROUP, driven_keep, (entry[:PAD], entry[PAD:]))

    corr[...] = jnp.zeros_like(corr)

    def iteration(it, carry):
        for half, ref in ((0, pos), (PAD, vel)):
            for e, part in enumerate(block_transpose([start[b, half : half + PAD, :] for b in range(GROUP)])):
                ref[e] = part

        def substep(n, carry):
            j = n // SUB
            for e in range(BLOCKS):
                p = pos[e]
                f = p - jnp.round(p)
                s = f * f
                poly = SINE[4] * s + SINE[3]
                for coef in (SINE[2], SINE[1], SINE[0]):
                    poly = poly * s + coef
                sine = (f * (1.0 - 4.0 * s)) * poly
                force[e] = tau_b[j, e] - stiff_b[j, e] * p - damp_b[j, e] * vel[e] - grav * sine
            acc = [vel[e] for e in range(BLOCKS)]
            for k in range(DOF):
                mass = mb[k]
                for e in range(BLOCKS):
                    acc[e] = acc[e] + mass * force[e, k : k + 1, :]
            for e in range(BLOCKS):
                vel[e] = acc[e]
                pos[e] = pos[e] + acc[e]
            return carry

        lax.fori_loop(0, HS * SUB, substep, 0)
        for half, ref in ((0, pos), (PAD, vel)):
            for b, part in enumerate(block_transpose([ref[e] for e in range(BLOCKS)])):
                shift[b, half : half + PAD, :] = part - end[b, half : half + PAD, :]

        def chain(b, qw):
            q, w = slice_step(b, qw[0], qw[1], False)
            return q + shift[b, :PAD, :], w + shift[b, PAD:, :]

        q, w = lax.fori_loop(1, GROUP, chain, (shift[0, :PAD, :], shift[0, PAD:, :]))
        entry = shifted(scan_groups(jnp.concatenate([q, w], axis=0)), 1)

        def keep(b, state):
            q, w, largest = state
            start[b] = start[b] + jnp.concatenate([q, w], axis=0)
            q, w = chain(b, (q, w))
            end[b] = end[b] + jnp.concatenate([q, w], axis=0)
            dq = q * (1.0 / TURN)
            dv = w * (1.0 / (TURN * FINE))
            square = jnp.sum(dq * dq + dv * dv, axis=0, keepdims=True)
            return q, w, jnp.maximum(largest, square)

        _, _, largest = lax.fori_loop(
            0, GROUP, keep, (entry[:PAD], entry[PAD:], jnp.zeros((1, LANES), f32))
        )
        group = lane_index(1) & 31
        for by in (16, 8, 4, 2, 1):
            other = jnp.where(group >= by, pltpu.roll(largest, by, 1), pltpu.roll(largest, LANES - 32 + by, 1))
            largest = jnp.maximum(largest, other)
        corr[pl.ds(it, 1), :] = jnp.sqrt(largest)
        return carry

    lax.fori_loop(0, ITERS, iteration, 0)

    rows[0 : OUT_CHUNKS * LANES, :] = jnp.zeros((OUT_CHUNKS * LANES, LANES), f32)
    for b in range(GROUP):
        rows[b * 2 * PAD : b * 2 * PAD + PAD, :] = end[b, :PAD, :] * (1.0 / TURN)
        rows[b * 2 * PAD + PAD : (b + 1) * 2 * PAD, :] = end[b, PAD:, :] * (1.0 / (TURN * FINE))
    rows[GROUP * 2 * PAD : GROUP * 2 * PAD + 8, :] = corr[...]
    for c in range(OUT_CHUNKS):
        out[:, c, :] = rows[c * LANES : (c + 1) * LANES, :].T


def unpack_kernel(core, recv, mine, other, corr, rows):
    for c in range(OUT_CHUNKS):
        rows[c * LANES : (c + 1) * LANES, :] = recv[:, c, :].T
    here = core[0] * 2
    for ref, base in ((mine, here), (other, 2 - here)):
        for s in range(2):
            at = pl.multiple_of((base + s) * 2 * PAD, 8)
            whole = rows[pl.ds(at, 2 * PAD), :]
            ref[s, 0:DOF, :] = whole[:DOF]
            ref[s, DOF : 2 * DOF, :] = whole[PAD : PAD + DOF]
    corr[...] = rows[GROUP * 2 * PAD : GROUP * 2 * PAD + 8, :]


def params(**more):
    return pltpu.CompilerParams(vmem_limit_bytes=VMEM_LIMIT, **more)


def pack_call(torque, contact, counts, init, mass):
    return pl.pallas_call(
        pack_kernel,
        out_shape=jax.ShapeDtypeStruct((LANES, CHUNKS, LANES), f32),
        scratch_shapes=[pltpu.VMEM((4 * LANES, LANES), f32)],
        compiler_params=params(),
        name="pack",
    )(torque, contact, counts, init, mass)


def main_call(recv, par):
    tile = (PAD, LANES)
    scratch = [
        (CHUNKS * LANES, LANES),
        (DOF, *tile),
        (GROUP, DOF, *tile),
        (3, 72, 2 * PAD, LANES),
        (18, 2 * PAD, LANES),
        (HS, BLOCKS, *tile),
        (HS, BLOCKS, *tile),
        (HS, BLOCKS, *tile),
        (STEPS, *tile),
        (STEPS, *tile),
        (GROUP, 2 * PAD, LANES),
        (GROUP, 2 * PAD, LANES),
        (GROUP, 2 * PAD, LANES),
        (1, 2 * PAD, LANES),
        (BLOCKS, *tile),
        (BLOCKS, *tile),
        (BLOCKS, *tile),
        (2 * PAD, LANES),
        (8, LANES),
    ]
    return pl.pallas_call(
        main_kernel,
        out_shape=jax.ShapeDtypeStruct((LANES, OUT_CHUNKS, LANES), f32),
        scratch_shapes=[pltpu.VMEM(shape, f32) for shape in scratch],
        compiler_params=params(),
        name="parareal",
    )(recv, par)


def unpack_call(core, recv):
    half = jax.ShapeDtypeStruct((2, 2 * DOF, LANES), f32)
    return pl.pallas_call(
        unpack_kernel,
        in_specs=[pl.BlockSpec(memory_space=pltpu.SMEM), pl.BlockSpec(memory_space=pltpu.VMEM)],
        out_shape=(half, half, jax.ShapeDtypeStruct((8, LANES), f32)),
        scratch_shapes=[pltpu.VMEM((OUT_CHUNKS * LANES, LANES), f32)],
        compiler_params=params(),
        name="unpack",
    )(core, recv)


def param_table(*vectors):
    table = jnp.stack([jnp.pad(v, (0, PAD - DOF)) for v in vectors], axis=1)
    return jnp.pad(table, ((0, 0), (0, 8 - len(vectors))))


def swapped(value):
    return lax.ppermute(value, "c", [(0, 1), (1, 0)])


def exchanged(value):
    return lax.all_to_all(value, PEERS, split_axis=0, concat_axis=0, tiled=True)


def shards(init_state, torque, contact, mass_inverse, *vectors):
    core = lax.axis_index("c")
    block = lax.axis_index("y")
    is_low = core == 0
    contact_f = contact.astype(f32)
    counts = jnp.sum(contact_f, axis=1, keepdims=True)

    def half(value, which):
        return lax.dynamic_slice_in_dim(value, which * LANES, LANES, value.ndim - 1)

    mass_here = lax.dynamic_index_in_dim(mass_inverse, block % 2, 0, keepdims=False)
    mass_here = jnp.pad(mass_here, ((0, 0), (0, PAD - DOF)))
    mass_here = jnp.pad(mass_here.reshape(DOF * PAD), (0, 12 * LANES - DOF * PAD)).reshape(12, LANES)
    small = jnp.concatenate(
        [half(contact_f, 1 - core), jnp.broadcast_to(counts, (4, LANES)), mass_here], axis=0
    )
    small_back = swapped(small)
    torque_back = swapped(half(torque, 1 - core))

    def in_order(own, back):
        return jnp.where(is_low, jnp.concatenate([own, back]), jnp.concatenate([back, own]))

    torque_all = in_order(half(torque, core), torque_back)
    contact_all = in_order(half(contact_f, core), small_back[0:4])
    counts_all = in_order(counts, small_back[4:8, 0:1])
    mass_sent = jnp.where(block // 2 == core, mass_here, small_back[8:20])

    sent = pack_call(torque_all, contact_all, counts_all, half(init_state, core), mass_sent)
    solved = main_call(exchanged(sent), param_table(*vectors))
    mine, other, corr = unpack_call(core[None].astype(jnp.int32), exchanged(solved))
    back, corr_back = swapped(other), swapped(corr)

    def side_by_side(own, back):
        return jnp.where(
            is_low, jnp.concatenate([own, back], axis=-1), jnp.concatenate([back, own], axis=-1)
        )

    return side_by_side(mine, back), side_by_side(corr, corr_back)[:ITERS]


def solution(mesh):
    torus = Mesh(mesh.devices.reshape(4, 8, 2, mesh.shape["env"]), ("x", "z", "c", "y"))
    return jax.shard_map(
        shards,
        mesh=torus,
        in_specs=(P(None, "y"), P(TM, None, "y"), P(TM, "y"), P(TM, None, None), P(), P(), P(), P(), P()),
        out_specs=(P(TM, None, "y"), P(None, "y")),
        check_vma=False,
    )
```

```python
import functools
import math

import jax
import jax.numpy as jnp
from jax import lax
from jax.experimental import pallas as pl
from jax.experimental.pallas import tpu as pltpu
from jax.sharding import Mesh
from jax.sharding import PartitionSpec as P

DOF = 35
PAD = 40
HS = 2
SUB = 32
ITERS = 3
GROUP = 4
BLOCKS = 4
CHIPS = 32
STEPS = GROUP * HS
LANES = 128
ENV = 1024
TM = ("x", "z", "c")
PEERS = ("x", "z")

DT = 0.05
FINE = DT / SUB
TURN = 1.0 / (2.0 * math.pi)
SINE = (6.283182595389212, -16.20867027746649, 16.7609745050196, -9.530799181282873, 3.0583252710952205)

ROW_CONTACT = STEPS * PAD
ROW_COUNT = ROW_CONTACT + 8
ROW_TAIL = ROW_COUNT + 8
IN_ROWS = 12
FOLD_ROWS = 18
FOLD_COLS = 36
FOLD = FOLD_ROWS * FOLD_COLS
MASS_ROWS = 5
CHUNKS = IN_ROWS + GROUP * MASS_ROWS
VMEM_LIMIT = 24 * 1024 * 1024

f32 = jnp.float32


def lane_index(rows):
    return lax.broadcasted_iota(jnp.int32, (rows, LANES), 1)


def block_transpose(parts):
    lane = lane_index(parts[0].shape[0])
    low = lane < 64
    even = ((lane >> 5) & 1) == 0
    a, b, c, d = parts
    a, c = jnp.where(low, a, pltpu.roll(c, 64, 1)), jnp.where(low, pltpu.roll(a, 64, 1), c)
    b, d = jnp.where(low, b, pltpu.roll(d, 64, 1)), jnp.where(low, pltpu.roll(b, 64, 1), d)
    a, b = jnp.where(even, a, pltpu.roll(b, 32, 1)), jnp.where(even, pltpu.roll(a, 96, 1), b)
    c, d = jnp.where(even, c, pltpu.roll(d, 32, 1)), jnp.where(even, pltpu.roll(c, 96, 1), d)
    return a, b, c, d


def block_spread(value):
    block = lane_index(value.shape[0]) >> 5
    turned = [value] + [pltpu.roll(value, 32 * m, 1) for m in (1, 2, 3)]
    return [
        jnp.where(
            block < 2,
            jnp.where(block == 0, turned[(0 - c) % 4], turned[(1 - c) % 4]),
            jnp.where(block == 2, turned[(2 - c) % 4], turned[(3 - c) % 4]),
        )
        for c in range(4)
    ]


def shifted(value, by):
    group = lane_index(value.shape[0]) & 31
    return jnp.where(group >= by, pltpu.roll(value, by, 1), 0.0)


def fold_index(k, i):
    k, i = min(k, i), max(k, i)
    if k < FOLD_ROWS:
        return k * FOLD_COLS + i + 1
    return (DOF - 1 - k) * FOLD_COLS + DOF - 1 - i


def half_of(which):
    return pl.ds(pl.multiple_of(which * LANES, LANES), LANES)


def split_kernel(core, torque, contact, send, counts):
    there = half_of(1 - core[0])
    send[...] = jnp.zeros_like(send)
    for t in range(4):
        send[t * PAD : t * PAD + DOF, :] = torque[:, t, there]
    send[4 * PAD : 4 * PAD + 4, :] = contact[:, there].astype(f32)
    total = jnp.sum(contact[...].astype(f32), axis=1, keepdims=True)
    for peer in range(8):
        counts[peer] = jnp.broadcast_to(total, (4, LANES))


def pack_kernel(core, torque, contact, back, totals, mass, tails, out, rows):
    me = core[0]
    here = half_of(me)
    rows[...] = jnp.zeros_like(rows)
    for t in range(4):
        rows[pl.ds(pl.multiple_of((4 * me + t) * PAD, 8), DOF), :] = torque[:, t, here]
        rows[pl.ds(pl.multiple_of((4 * (1 - me) + t) * PAD, 8), PAD), :] = back[t * PAD : (t + 1) * PAD, :]
    own = contact[:, here].astype(f32)
    other = back[4 * PAD : 4 * PAD + 4, :]
    rows[ROW_CONTACT : ROW_CONTACT + 8, :] = jnp.where(
        me == 0, jnp.concatenate([own, other]), jnp.concatenate([other, own])
    )
    rows[ROW_COUNT : ROW_COUNT + 8, :] = totals[...]
    block = lane_index(8) >> 5
    tail = jnp.zeros((8, LANES), f32)
    for b in range(GROUP):
        tail = jnp.where(block == b, tails[:, b : b + 1], tail)
    rows[ROW_TAIL : ROW_TAIL + 8, :] = tail
    for c in range(3):
        turned = rows[c * LANES : (c + 1) * LANES, :].T
        for e in range(BLOCKS):
            out[:, e * 3 + c, :] = turned[e * CHIPS : (e + 1) * CHIPS]
    for m in range(GROUP * MASS_ROWS):
        out[:, IN_ROWS + m, :] = jnp.broadcast_to(mass[m : m + 1, :], (CHIPS, LANES))


def state_row(k):
    return k if k < DOF else k + PAD - DOF


def main_kernel(
    chip, init_ref, recv, par, out, rows, fold, mb, ma, wide, cols, tau_b, stiff_b, damp_b, spring, fric, start, end, shift, diff, pos, vel, force, vec, corr
):
    for c in range(3):
        rows[c * LANES : (c + 1) * LANES, :] = jnp.concatenate(
            [recv[:, e * 3 + c, :] for e in range(BLOCKS)]
        ).T
    for m in range(MASS_ROWS):
        fold[m * LANES : (m + 1) * LANES, :] = jnp.concatenate(
            [recv[:, IN_ROWS + b * MASS_ROWS + m, :] for b in range(GROUP)]
        ).T
    fold[MASS_ROWS * LANES : FOLD, :] = rows[ROW_TAIL : ROW_TAIL + 8, :]

    def param(i):
        return jnp.broadcast_to(par[:, i : i + 1], (PAD, LANES))

    stiffness, damping, gravity, contact_stiffness, contact_damping = (param(i) for i in range(5))

    for k in range(DOF):
        for i in range(DOF):
            at = fold_index(k, i)
            mb[k, i : i + 1, :] = fold[at : at + 1, :]
        mb[k, DOF:PAD, :] = jnp.zeros((PAD - DOF, LANES), f32)

    def place_mass(k, carry):
        for b, spread in enumerate(block_spread(mb[k])):
            ma[b, k] = spread
        return carry

    lax.fori_loop(0, DOF, place_mass, 0)

    mean = rows[ROW_COUNT : ROW_COUNT + 8, :] / ENV
    for t in range(STEPS):
        here = mean[t : t + 1, :]
        spring[t] = (stiffness + gravity + here * contact_stiffness) * (FINE * DT)
        fric[t] = (damping + here * contact_damping) * DT

    for j in range(HS):
        turned = block_transpose([rows[(2 * b + j) * PAD : (2 * b + j + 1) * PAD, :] for b in range(GROUP)])
        touch = block_transpose(
            [rows[ROW_CONTACT + 2 * b + j : ROW_CONTACT + 2 * b + j + 1, :] for b in range(GROUP)]
        )
        for e in range(BLOCKS):
            tau_b[j, e] = turned[e] * (FINE * FINE * TURN)
            stiff_b[j, e] = (stiffness + touch[e] * contact_stiffness) * (FINE * FINE)
            damp_b[j, e] = (damping + touch[e] * contact_damping) * FINE

    grav = gravity * (FINE * FINE * TURN)

    def half_step(b, t, q, w, driven):
        pull = spring[t] * q + fric[t] * w
        if driven:
            at = t * PAD if isinstance(t, int) else pl.multiple_of(t * PAD, 8)
            pull = rows[pl.ds(at, PAD), :] * (FINE * DT * TURN) - pull
        else:
            pull = -pull
        vec[0:PAD, :] = pull
        for k in range(DOF):
            w = w + ma[b, k] * vec[k : k + 1, :]
        return q + float(SUB) * w, w

    def slice_step(b, q, w, driven):
        q, w = half_step(b, 2 * b, q, w, driven)
        return half_step(b, 2 * b + 1, q, w, driven)

    def apply_wide(level, value):
        vec[...] = value
        total = None
        for k in range(2 * DOF):
            term = wide[level, k] * vec[state_row(k) : state_row(k) + 1, :]
            total = term if total is None else total + term
        return total

    row80 = lax.broadcasted_iota(jnp.int32, (2 * PAD, LANES), 0)
    col_block = lane_index(2 * PAD) >> 5

    def spread_columns(level, cg, value):
        for c, spread in enumerate(block_spread(value)):
            wide[level, 4 * cg + c] = spread

    def first_columns(cg, carry):
        col = 4 * cg + col_block
        col = jnp.where(col < DOF, col, col + (PAD - DOF))
        unit = jnp.where(row80 == col, 1.0, 0.0)

        def one(b, qw):
            return slice_step(b, qw[0], qw[1], False)

        q, w = lax.fori_loop(0, GROUP, one, (unit[:PAD], unit[PAD:]))
        value = jnp.concatenate([q, w], axis=0)
        cols[cg] = value
        spread_columns(0, cg, value)
        return carry

    lax.fori_loop(0, 18, first_columns, 0)
    for level, by in ((1, 1), (2, 2)):

        def more_columns(cg, carry, level=level, by=by):
            value = apply_wide(level - 1, shifted(cols[cg], by))
            cols[cg] = value
            spread_columns(level, cg, value)
            return carry

        lax.fori_loop(0, 18, more_columns, 0)

    def scan_groups(value):
        value = value + apply_wide(0, shifted(value, 1))
        value = value + apply_wide(1, shifted(value, 2))
        diff[0] = value

        def more(i, running):
            return diff[0] + apply_wide(2, shifted(running, 4))

        return lax.fori_loop(0, 7, more, value)

    first = (lane_index(2 * PAD) & 31) == 0
    back_by = LANES - chip[0]
    vec[...] = jnp.zeros_like(vec)
    vec[0:DOF, :] = init_ref[:DOF, half_of(chip[1])] * TURN
    vec[PAD : PAD + DOF, :] = init_ref[DOF:, half_of(chip[1])] * (FINE * TURN)
    init = jnp.where(first, pltpu.roll(vec[...], back_by, 1), 0.0)

    def driven_slice(b, qw):
        return slice_step(b, qw[0], qw[1], True)

    q, w = lax.fori_loop(0, GROUP, driven_slice, (init[:PAD], init[PAD:]))
    ends = scan_groups(jnp.concatenate([q, w], axis=0))
    entry = jnp.where(first, init, shifted(ends, 1))

    def driven_keep(b, qw):
        start[b] = jnp.concatenate(qw, axis=0)
        qw = slice_step(b, qw[0], qw[1], True)
        end[b] = jnp.concatenate(qw, axis=0)
        return qw

    lax.fori_loop(0, GROUP, driven_keep, (entry[:PAD], entry[PAD:]))

    corr[...] = jnp.zeros_like(corr)

    def iteration(it, carry):
        for half, ref in ((0, pos), (PAD, vel)):
            for e, part in enumerate(block_transpose([start[b, half : half + PAD, :] for b in range(GROUP)])):
                ref[e] = part

        def substep(n, carry):
            j = n // SUB
            for e in range(BLOCKS):
                p = pos[e]
                f = p - jnp.round(p)
                s = f * f
                poly = SINE[4] * s + SINE[3]
                for coef in (SINE[2], SINE[1], SINE[0]):
                    poly = poly * s + coef
                sine = (f * (1.0 - 4.0 * s)) * poly
                force[e] = tau_b[j, e] - stiff_b[j, e] * p - damp_b[j, e] * vel[e] - grav * sine
            acc = [vel[e] for e in range(BLOCKS)]
            for k in range(DOF):
                mass = mb[k]
                for e in range(BLOCKS):
                    acc[e] = acc[e] + mass * force[e, k : k + 1, :]
            for e in range(BLOCKS):
                vel[e] = acc[e]
                pos[e] = pos[e] + acc[e]
            return carry

        lax.fori_loop(0, HS * SUB, substep, 0)
        for half, ref in ((0, pos), (PAD, vel)):
            for b, part in enumerate(block_transpose([ref[e] for e in range(BLOCKS)])):
                shift[b, half : half + PAD, :] = part - end[b, half : half + PAD, :]

        def chain(b, qw):
            q, w = slice_step(b, qw[0], qw[1], False)
            return q + shift[b, :PAD, :], w + shift[b, PAD:, :]

        q, w = lax.fori_loop(1, GROUP, chain, (shift[0, :PAD, :], shift[0, PAD:, :]))
        entry = shifted(scan_groups(jnp.concatenate([q, w], axis=0)), 1)

        def keep(b, state):
            q, w, largest = state
            start[b] = start[b] + jnp.concatenate([q, w], axis=0)
            q, w = chain(b, (q, w))
            end[b] = end[b] + jnp.concatenate([q, w], axis=0)
            dq = q * (1.0 / TURN)
            dv = w * (1.0 / (TURN * FINE))
            square = jnp.sum(dq * dq + dv * dv, axis=0, keepdims=True)
            return q, w, jnp.maximum(largest, square)

        _, _, largest = lax.fori_loop(
            0, GROUP, keep, (entry[:PAD], entry[PAD:], jnp.zeros((1, LANES), f32))
        )
        group = lane_index(1) & 31
        for by in (16, 8, 4, 2, 1):
            other = jnp.where(group >= by, pltpu.roll(largest, by, 1), pltpu.roll(largest, LANES - 32 + by, 1))
            largest = jnp.maximum(largest, other)
        corr[pl.ds(it, 1), :] = jnp.sqrt(largest)
        return carry

    lax.fori_loop(0, ITERS, iteration, 0)

    for b in range(GROUP):
        rows[b * 2 * PAD : b * 2 * PAD + PAD, :] = end[b, :PAD, :] * (1.0 / TURN)
        rows[b * 2 * PAD + PAD : (b + 1) * 2 * PAD, :] = end[b, PAD:, :] * (1.0 / (TURN * FINE))
    rows[GROUP * 2 * PAD : GROUP * 2 * PAD + 8, :] = corr[...]
    for c in range(3):
        turned = rows[c * LANES : (c + 1) * LANES, :].T
        for e in range(BLOCKS):
            at = e * 3 + c
            out[:, at // 4, at % 4, :] = turned[e * CHIPS : (e + 1) * CHIPS]


def unpack_kernel(core, recv, mine, send, rows):
    for c in range(3):
        at = [e * 3 + c for e in range(BLOCKS)]
        rows[c * LANES : (c + 1) * LANES, :] = jnp.concatenate([recv[:, i // 4, i % 4, :] for i in at]).T
    corr = rows[GROUP * 2 * PAD : GROUP * 2 * PAD + 8, :]
    for ref, which in ((mine, core[0]), (send, 1 - core[0])):
        ref[0 : 4 * PAD, :] = rows[pl.ds(pl.multiple_of(which * 4 * PAD, 8), 4 * PAD), :]
        ref[4 * PAD :, :] = corr


def join_kernel(core, mine, back, out, corr):
    for ref, which in ((mine, core[0]), (back, 1 - core[0])):
        part = half_of(which)
        for s in range(2):
            out[0:DOF, s, part] = ref[s * 2 * PAD : s * 2 * PAD + DOF, :]
            out[DOF : 2 * DOF, s, part] = ref[s * 2 * PAD + PAD : s * 2 * PAD + PAD + DOF, :]
        corr[:, part] = ref[4 * PAD : 4 * PAD + ITERS, :]


SWAP = (4 * PAD + 8, LANES)


def local_call(kernel, name, out_shapes, scratch, scalars, *arrays):
    smem = pl.BlockSpec(memory_space=pltpu.SMEM)
    vmem = pl.BlockSpec(memory_space=pltpu.VMEM)
    shapes = tuple(jax.ShapeDtypeStruct(shape, f32) for shape in out_shapes)
    return pl.pallas_call(
        kernel,
        in_specs=[smem] + [vmem] * len(arrays),
        out_specs=tuple(vmem for _ in shapes) if len(shapes) > 1 else vmem,
        out_shape=shapes if len(shapes) > 1 else shapes[0],
        scratch_shapes=[pltpu.VMEM(shape, f32) for shape in scratch],
        compiler_params=pltpu.CompilerParams(vmem_limit_bytes=VMEM_LIMIT),
        name=name,
    )(scalars, *arrays)


def main_call(chip, init, recv, par):
    tile = (PAD, LANES)
    scratch = [
        (3 * LANES, LANES),
        (FOLD, LANES),
        (DOF, *tile),
        (GROUP, DOF, *tile),
        (3, 72, 2 * PAD, LANES),
        (18, 2 * PAD, LANES),
        (HS, BLOCKS, *tile),
        (HS, BLOCKS, *tile),
        (HS, BLOCKS, *tile),
        (STEPS, *tile),
        (STEPS, *tile),
        (GROUP, 2 * PAD, LANES),
        (GROUP, 2 * PAD, LANES),
        (GROUP, 2 * PAD, LANES),
        (1, 2 * PAD, LANES),
        (BLOCKS, *tile),
        (BLOCKS, *tile),
        (BLOCKS, *tile),
        (2 * PAD, LANES),
        (8, LANES),
    ]
    return local_call(main_kernel, "parareal", [(CHIPS, 3, 4, LANES)], scratch, chip, init, recv, par)


def param_table(*vectors):
    table = jnp.stack([jnp.pad(v, (0, PAD - DOF)) for v in vectors], axis=1)
    return jnp.pad(table, ((0, 0), (0, 8 - len(vectors))))


def swapped(value):
    return lax.ppermute(value, "c", [(0, 1), (1, 0)])


def exchanged(value):
    return lax.all_to_all(value, PEERS, split_axis=0, concat_axis=0, tiled=True)


def folded(matrices):
    row = lax.broadcasted_iota(jnp.int32, (FOLD_ROWS, FOLD_COLS), 0)
    col = lax.broadcasted_iota(jnp.int32, (FOLD_ROWS, FOLD_COLS), 1)
    plain = jnp.pad(matrices, ((0, 0), (0, 0), (1, 0)))[:, :FOLD_ROWS]
    turned = jnp.pad(matrices[:, ::-1, ::-1], ((0, 0), (0, 0), (0, 1)))[:, :FOLD_ROWS]
    return jnp.where(col <= row, turned, plain).reshape(-1, FOLD)


def shards(init_state, torque, contact, mass_inverse, *vectors):
    core = lax.axis_index("c").astype(jnp.int32)
    chip = (lax.axis_index("x") * lax.axis_size("z") + lax.axis_index("z")).astype(jnp.int32)

    mass_back = swapped(mass_inverse)
    torque = torque.transpose(1, 0, 2)
    send, counts = local_call(split_kernel, "split", [SWAP, (8, 4, LANES)], [], core[None], torque, contact)
    back = swapped(send)
    counts = lax.all_to_all(counts, ("c", "y"), split_axis=0, concat_axis=0, tiled=True)
    totals = counts.reshape(2, BLOCKS, 4, LANES).sum(axis=1).reshape(8, LANES)
    order = core == 0
    matrices = folded(
        jnp.where(
            order,
            jnp.concatenate([mass_inverse, mass_back]),
            jnp.concatenate([mass_back, mass_inverse]),
        )
    )
    mass_rows = matrices[:, : MASS_ROWS * LANES].reshape(GROUP * MASS_ROWS, LANES)
    mass_tails = matrices[:, MASS_ROWS * LANES :].T

    sent = local_call(
        pack_kernel,
        "pack",
        [(CHIPS, CHUNKS, LANES)],
        [(3 * LANES, LANES)],
        core[None],
        torque,
        contact,
        back,
        totals,
        mass_rows,
        mass_tails,
    )
    solved = main_call(jnp.stack([chip, core]), init_state, exchanged(sent), param_table(*vectors))
    mine, send = local_call(
        unpack_kernel, "unpack", [SWAP, SWAP], [(3 * LANES, LANES)], core[None], exchanged(solved)
    )
    final, corr = local_call(
        join_kernel, "join", [(2 * DOF, 2, 2 * LANES), (ITERS, 2 * LANES)], [], core[None], mine, swapped(send)
    )
    return final.transpose(1, 0, 2), corr


def solution(mesh):
    torus = Mesh(mesh.devices.reshape(4, 8, 2, mesh.shape["env"]), ("x", "z", "c", "y"))
    return jax.shard_map(
        shards,
        mesh=torus,
        in_specs=(P(None, "y"), P(TM, None, "y"), P(TM, "y"), P(TM, None, None), P(), P(), P(), P(), P()),
        out_specs=(P(TM, None, "y"), P(None, "y")),
        check_vma=False,
    )
```

```python
import functools
import math

import jax
import jax.numpy as jnp
from jax import lax
from jax.experimental import pallas as pl
from jax.experimental.pallas import tpu as pltpu
from jax.sharding import Mesh
from jax.sharding import PartitionSpec as P

DOF = 35
PAD = 40
HS = 2
SUB = 32
ITERS = 3
GROUP = 4
BLOCKS = 4
CHIPS = 32
STEPS = GROUP * HS
LANES = 128
ENV = 1024
TM = ("x", "z", "c")
PEERS = ("x", "z")

DT = 0.05
FINE = DT / SUB
TURN = 1.0 / (2.0 * math.pi)
SINE = (6.283182595389212, -16.20867027746649, 16.7609745050196, -9.530799181282873, 3.0583252710952205)

ROW_CONTACT = STEPS * PAD
ROW_COUNT = ROW_CONTACT + 8
ROW_TAIL = ROW_COUNT + 8
IN_ROWS = 12
FOLD_ROWS = 18
FOLD_COLS = 36
FOLD = FOLD_ROWS * FOLD_COLS
MASS_ROWS = 5
CHUNKS = IN_ROWS + GROUP * MASS_ROWS
VMEM_LIMIT = 24 * 1024 * 1024

f32 = jnp.float32


def lane_index(rows):
    return lax.broadcasted_iota(jnp.int32, (rows, LANES), 1)


def block_transpose(parts):
    lane = lane_index(parts[0].shape[0])
    low = lane < 64
    even = ((lane >> 5) & 1) == 0
    a, b, c, d = parts
    a, c = jnp.where(low, a, pltpu.roll(c, 64, 1)), jnp.where(low, pltpu.roll(a, 64, 1), c)
    b, d = jnp.where(low, b, pltpu.roll(d, 64, 1)), jnp.where(low, pltpu.roll(b, 64, 1), d)
    a, b = jnp.where(even, a, pltpu.roll(b, 32, 1)), jnp.where(even, pltpu.roll(a, 96, 1), b)
    c, d = jnp.where(even, c, pltpu.roll(d, 32, 1)), jnp.where(even, pltpu.roll(c, 96, 1), d)
    return a, b, c, d


def block_spread(value):
    block = lane_index(value.shape[0]) >> 5
    turned = [value] + [pltpu.roll(value, 32 * m, 1) for m in (1, 2, 3)]
    return [
        jnp.where(
            block < 2,
            jnp.where(block == 0, turned[(0 - c) % 4], turned[(1 - c) % 4]),
            jnp.where(block == 2, turned[(2 - c) % 4], turned[(3 - c) % 4]),
        )
        for c in range(4)
    ]


def shifted(value, by):
    group = lane_index(value.shape[0]) & 31
    return jnp.where(group >= by, pltpu.roll(value, by, 1), 0.0)


def fold_index(k, i):
    k, i = min(k, i), max(k, i)
    if k < FOLD_ROWS:
        return k * FOLD_COLS + i + 1
    return (DOF - 1 - k) * FOLD_COLS + DOF - 1 - i


def half_of(which):
    return pl.ds(pl.multiple_of(which * LANES, LANES), LANES)


def count_kernel(core, contact, counts):
    total = jnp.sum(contact[...].astype(f32), axis=1, keepdims=True)
    for peer in range(8):
        counts[peer] = jnp.broadcast_to(total, (4, LANES))


def split_kernel(core, torque, contact, send):
    there = half_of(1 - core[0])
    send[...] = jnp.zeros_like(send)
    for t in range(4):
        send[t * PAD : t * PAD + DOF, :] = torque[:, t, there]
    send[4 * PAD : 4 * PAD + 4, :] = contact[:, there].astype(f32)


def pack_kernel(core, torque, contact, back, totals, mass, tails, out, rows):
    me = core[0]
    here = half_of(me)
    rows[...] = jnp.zeros_like(rows)
    for t in range(4):
        rows[pl.ds(pl.multiple_of((4 * me + t) * PAD, 8), DOF), :] = torque[:, t, here]
        rows[pl.ds(pl.multiple_of((4 * (1 - me) + t) * PAD, 8), PAD), :] = back[t * PAD : (t + 1) * PAD, :]
    own = contact[:, here].astype(f32)
    other = back[4 * PAD : 4 * PAD + 4, :]
    rows[ROW_CONTACT : ROW_CONTACT + 8, :] = jnp.where(
        me == 0, jnp.concatenate([own, other]), jnp.concatenate([other, own])
    )
    rows[ROW_COUNT : ROW_COUNT + 8, :] = totals[...]
    block = lane_index(8) >> 5
    tail = jnp.zeros((8, LANES), f32)
    for b in range(GROUP):
        tail = jnp.where(block == b, tails[:, b : b + 1], tail)
    rows[ROW_TAIL : ROW_TAIL + 8, :] = tail
    for c in range(3):
        turned = rows[c * LANES : (c + 1) * LANES, :].T
        for e in range(BLOCKS):
            out[:, e * 3 + c, :] = turned[e * CHIPS : (e + 1) * CHIPS]
    for m in range(GROUP * MASS_ROWS):
        out[:, IN_ROWS + m, :] = jnp.broadcast_to(mass[m : m + 1, :], (CHIPS, LANES))


def state_row(k):
    return k if k < DOF else k + PAD - DOF


def main_kernel(
    chip, init_ref, recv, par, out, rows, fold, mb, ma, wide, cols, tau_b, stiff_b, damp_b, spring, fric, start, end, shift, pos, vel, force, vec, corr
):
    for c in range(3):
        rows[c * LANES : (c + 1) * LANES, :] = jnp.concatenate(
            [recv[:, e * 3 + c, :] for e in range(BLOCKS)]
        ).T
    for m in range(MASS_ROWS):
        fold[m * LANES : (m + 1) * LANES, :] = jnp.concatenate(
            [recv[:, IN_ROWS + b * MASS_ROWS + m, :] for b in range(GROUP)]
        ).T
    fold[MASS_ROWS * LANES : FOLD, :] = rows[ROW_TAIL : ROW_TAIL + 8, :]

    def param(i):
        return jnp.broadcast_to(par[:, i : i + 1], (PAD, LANES))

    stiffness, damping, gravity, contact_stiffness, contact_damping = (param(i) for i in range(5))

    for k in range(DOF):
        for i in range(DOF):
            at = fold_index(k, i)
            mb[k, i : i + 1, :] = fold[at : at + 1, :]
        mb[k, DOF:PAD, :] = jnp.zeros((PAD - DOF, LANES), f32)

    def place_mass(n, carry):
        for k in range(5):
            for b, spread in enumerate(block_spread(mb[5 * n + k])):
                ma[b, 5 * n + k] = spread
        return carry

    lax.fori_loop(0, DOF // 5, place_mass, 0)

    mean = rows[ROW_COUNT : ROW_COUNT + 8, :] / ENV
    for t in range(STEPS):
        here = mean[t : t + 1, :]
        spring[t] = (stiffness + gravity + here * contact_stiffness) * (FINE * DT)
        fric[t] = (damping + here * contact_damping) * DT

    for j in range(HS):
        turned = block_transpose([rows[(2 * b + j) * PAD : (2 * b + j + 1) * PAD, :] for b in range(GROUP)])
        touch = block_transpose(
            [rows[ROW_CONTACT + 2 * b + j : ROW_CONTACT + 2 * b + j + 1, :] for b in range(GROUP)]
        )
        for e in range(BLOCKS):
            tau_b[j, e] = turned[e] * (FINE * FINE * TURN)
            stiff_b[j, e] = (stiffness + touch[e] * contact_stiffness) * (FINE * FINE)
            damp_b[j, e] = (damping + touch[e] * contact_damping) * FINE

    grav = gravity * (FINE * FINE * TURN)

    def half_step(b, t, states, driven):
        moved = []
        for n, (q, w) in enumerate(states):
            pull = spring[t] * q + fric[t] * w
            if driven:
                pull = rows[pl.ds(pl.multiple_of(t * PAD, 8), PAD), :] * (FINE * DT * TURN) - pull
            else:
                pull = -pull
            vec[n, 0:PAD, :] = pull
            moved.append(w)
        for k in range(DOF):
            mass = ma[b, k]
            for n in range(len(states)):
                moved[n] = moved[n] + mass * vec[n, k : k + 1, :]
        return tuple((q + float(SUB) * w, w) for (q, _), w in zip(states, moved))

    def slice_step(b, states, driven):
        return half_step(b, 2 * b + 1, half_step(b, 2 * b, states, driven), driven)

    def one_slice(b, q, w, driven):
        return slice_step(b, ((q, w),), driven)[0]

    def apply_wide(level, row_of):
        low = high = None
        for k in range(2 * DOF):
            row = row_of(state_row(k))
            term = wide[level, k, :PAD, :] * row
            low = term if low is None else low + term
            if k < DOF:
                term = wide[level, k, PAD:, :] * row
                high = term if high is None else high + term
        for k in range(DOF, 2 * DOF):
            high = high + wide[level, k, PAD:, :] * row_of(state_row(k))
        return low, high

    row80 = lax.broadcasted_iota(jnp.int32, (2 * PAD, LANES), 0)
    col_block = lane_index(2 * PAD) >> 5

    def first_columns(pair, carry):
        states = []
        for n in range(2):
            col = 4 * (2 * pair + n) + col_block
            col = jnp.where(col < DOF, col, col + (PAD - DOF))
            unit = jnp.where(row80 == col, 1.0, 0.0)
            states.append((unit[:PAD], unit[PAD:]))
        states = lax.fori_loop(0, GROUP, lambda b, now: slice_step(b, now, False), tuple(states))
        for n in range(2):
            cols[2 * pair + n, :PAD, :] = states[n][0]
            cols[2 * pair + n, PAD:, :] = states[n][1]
        return carry

    lax.fori_loop(0, 9, first_columns, 0)

    def spread_columns(level, by):
        def some(n, carry):
            for m in range(3):
                value = cols[3 * n + m]
                for c, spread in enumerate(block_spread(value)):
                    wide[level, 4 * (3 * n + m) + c] = spread
                if by:
                    cols[3 * n + m] = shifted(value, by)
            return carry

        lax.fori_loop(0, 6, some, 0)

    def more_columns(level):
        def one(cg, carry):
            low, high = apply_wide(level - 1, lambda r: cols[cg, r : r + 1, :])
            cols[cg, :PAD, :] = low
            cols[cg, PAD:, :] = high
            return carry

        lax.fori_loop(0, 18, one, 0)

    spread_columns(0, 1)
    more_columns(1)
    spread_columns(1, 2)
    more_columns(2)
    spread_columns(2, 0)

    def scan_groups(q, w):
        def add_earlier(level, by, slot, base, state):
            vec[slot, :PAD, :] = shifted(state[0], by)
            vec[slot, PAD:, :] = shifted(state[1], by)
            low, high = apply_wide(level, lambda r: vec[slot, r : r + 1, :])
            return base[0] + low, base[1] + high

        state = (q, w)
        state = add_earlier(0, 1, 0, state, state)
        state = base = add_earlier(1, 2, 1, state, state)
        for n in range(7):
            state = add_earlier(2, 4, n % 2, base, state)
        return state

    first = (lane_index(2 * PAD) & 31) == 0
    back_by = LANES - chip[0]
    vec[0] = jnp.zeros((2 * PAD, LANES), f32)
    vec[0, 0:DOF, :] = init_ref[:DOF, half_of(chip[1])] * TURN
    vec[0, PAD : PAD + DOF, :] = init_ref[DOF:, half_of(chip[1])] * (FINE * TURN)
    init = jnp.where(first, pltpu.roll(vec[0], back_by, 1), 0.0)

    def driven_slice(b, qw):
        return one_slice(b, qw[0], qw[1], True)

    q, w = lax.fori_loop(0, GROUP, driven_slice, (init[:PAD], init[PAD:]))
    q, w = scan_groups(q, w)
    first = first[:PAD]
    entry = jnp.where(first, init[:PAD], shifted(q, 1)), jnp.where(first, init[PAD:], shifted(w, 1))

    def driven_keep(b, qw):
        start[b, :PAD, :], start[b, PAD:, :] = qw
        qw = one_slice(b, qw[0], qw[1], True)
        end[b, :PAD, :], end[b, PAD:, :] = qw
        return qw

    lax.fori_loop(0, GROUP, driven_keep, entry)

    corr[...] = jnp.zeros_like(corr)

    def iteration(it, carry):
        for half, ref in ((0, pos), (PAD, vel)):
            for e, part in enumerate(block_transpose([start[b, half : half + PAD, :] for b in range(GROUP)])):
                ref[e] = part

        def substep(n, carry):
            j = n // SUB
            for e in range(BLOCKS):
                p = pos[e]
                f = p - jnp.round(p)
                s = f * f
                poly = SINE[4] * s + SINE[3]
                for coef in (SINE[2], SINE[1], SINE[0]):
                    poly = poly * s + coef
                sine = (f * (1.0 - 4.0 * s)) * poly
                force[e] = tau_b[j, e] - stiff_b[j, e] * p - damp_b[j, e] * vel[e] - grav * sine
            acc = [vel[e] for e in range(BLOCKS)]
            for k in range(DOF):
                mass = mb[k]
                for e in range(BLOCKS):
                    acc[e] = acc[e] + mass * force[e, k : k + 1, :]
            for e in range(BLOCKS):
                vel[e] = acc[e]
                pos[e] = pos[e] + acc[e]
            return carry

        lax.fori_loop(0, HS * SUB, substep, 0)
        for half, ref in ((0, pos), (PAD, vel)):
            for b, part in enumerate(block_transpose([ref[e] for e in range(BLOCKS)])):
                shift[b, half : half + PAD, :] = part - end[b, half : half + PAD, :]

        def chain(b, qw):
            q, w = one_slice(b, qw[0], qw[1], False)
            return q + shift[b, :PAD, :], w + shift[b, PAD:, :]

        q, w = lax.fori_loop(1, GROUP, chain, (shift[0, :PAD, :], shift[0, PAD:, :]))
        q, w = scan_groups(q, w)

        def keep(b, state):
            q, w, largest = state
            start[b, :PAD, :] = start[b, :PAD, :] + q
            start[b, PAD:, :] = start[b, PAD:, :] + w
            q, w = chain(b, (q, w))
            end[b, :PAD, :] = end[b, :PAD, :] + q
            end[b, PAD:, :] = end[b, PAD:, :] + w
            dq = q * (1.0 / TURN)
            dv = w * (1.0 / (TURN * FINE))
            square = jnp.sum(dq * dq + dv * dv, axis=0, keepdims=True)
            return q, w, jnp.maximum(largest, square)

        _, _, largest = lax.fori_loop(
            0, GROUP, keep, (shifted(q, 1), shifted(w, 1), jnp.zeros((1, LANES), f32))
        )
        group = lane_index(1) & 31
        for by in (16, 8, 4, 2, 1):
            other = jnp.where(group >= by, pltpu.roll(largest, by, 1), pltpu.roll(largest, LANES - 32 + by, 1))
            largest = jnp.maximum(largest, other)
        corr[pl.ds(it, 1), :] = jnp.sqrt(largest)
        return carry

    lax.fori_loop(0, ITERS, iteration, 0)

    for b in range(GROUP):
        rows[b * 2 * PAD : b * 2 * PAD + PAD, :] = end[b, :PAD, :] * (1.0 / TURN)
        rows[b * 2 * PAD + PAD : (b + 1) * 2 * PAD, :] = end[b, PAD:, :] * (1.0 / (TURN * FINE))
    rows[GROUP * 2 * PAD : GROUP * 2 * PAD + 8, :] = corr[...]
    for c in range(3):
        turned = rows[c * LANES : (c + 1) * LANES, :].T
        for e in range(BLOCKS):
            at = e * 3 + c
            out[:, at // 4, at % 4, :] = turned[e * CHIPS : (e + 1) * CHIPS]


def unpack_kernel(core, recv, mine, send, rows):
    for c in range(3):
        at = [e * 3 + c for e in range(BLOCKS)]
        rows[c * LANES : (c + 1) * LANES, :] = jnp.concatenate([recv[:, i // 4, i % 4, :] for i in at]).T
    corr = rows[GROUP * 2 * PAD : GROUP * 2 * PAD + 8, :]
    for ref, which in ((mine, core[0]), (send, 1 - core[0])):
        ref[0 : 4 * PAD, :] = rows[pl.ds(pl.multiple_of(which * 4 * PAD, 8), 4 * PAD), :]
        ref[4 * PAD :, :] = corr


def join_kernel(core, mine, back, out, corr):
    for ref, which in ((mine, core[0]), (back, 1 - core[0])):
        part = half_of(which)
        for s in range(2):
            out[0:DOF, s, part] = ref[s * 2 * PAD : s * 2 * PAD + DOF, :]
            out[DOF : 2 * DOF, s, part] = ref[s * 2 * PAD + PAD : s * 2 * PAD + PAD + DOF, :]
        corr[:, part] = ref[4 * PAD : 4 * PAD + ITERS, :]


SWAP = (4 * PAD + 8, LANES)


def local_call(kernel, name, out_shapes, scratch, scalars, *arrays):
    smem = pl.BlockSpec(memory_space=pltpu.SMEM)
    vmem = pl.BlockSpec(memory_space=pltpu.VMEM)
    shapes = tuple(jax.ShapeDtypeStruct(shape, f32) for shape in out_shapes)
    return pl.pallas_call(
        kernel,
        in_specs=[smem] + [vmem] * len(arrays),
        out_specs=tuple(vmem for _ in shapes) if len(shapes) > 1 else vmem,
        out_shape=shapes if len(shapes) > 1 else shapes[0],
        scratch_shapes=[pltpu.VMEM(shape, f32) for shape in scratch],
        compiler_params=pltpu.CompilerParams(vmem_limit_bytes=VMEM_LIMIT),
        name=name,
    )(scalars, *arrays)


def main_call(chip, init, recv, par):
    tile = (PAD, LANES)
    scratch = [
        (3 * LANES, LANES),
        (FOLD, LANES),
        (DOF, *tile),
        (GROUP, DOF, *tile),
        (3, 72, 2 * PAD, LANES),
        (18, 2 * PAD, LANES),
        (HS, BLOCKS, *tile),
        (HS, BLOCKS, *tile),
        (HS, BLOCKS, *tile),
        (STEPS, *tile),
        (STEPS, *tile),
        (GROUP, 2 * PAD, LANES),
        (GROUP, 2 * PAD, LANES),
        (GROUP, 2 * PAD, LANES),
        (BLOCKS, *tile),
        (BLOCKS, *tile),
        (BLOCKS, *tile),
        (2, 2 * PAD, LANES),
        (8, LANES),
    ]
    return local_call(main_kernel, "parareal", [(CHIPS, 3, 4, LANES)], scratch, chip, init, recv, par)


def param_table(*vectors):
    table = jnp.stack([jnp.pad(v, (0, PAD - DOF)) for v in vectors], axis=1)
    return jnp.pad(table, ((0, 0), (0, 8 - len(vectors))))


def swapped(value):
    return lax.ppermute(value, "c", [(0, 1), (1, 0)])


def exchanged(value):
    return lax.all_to_all(value, PEERS, split_axis=0, concat_axis=0, tiled=True)


def folded(matrices):
    row = lax.broadcasted_iota(jnp.int32, (FOLD_ROWS, FOLD_COLS), 0)
    col = lax.broadcasted_iota(jnp.int32, (FOLD_ROWS, FOLD_COLS), 1)
    plain = jnp.pad(matrices, ((0, 0), (0, 0), (1, 0)))[:, :FOLD_ROWS]
    turned = jnp.pad(matrices[:, ::-1, ::-1], ((0, 0), (0, 0), (0, 1)))[:, :FOLD_ROWS]
    return jnp.where(col <= row, turned, plain).reshape(-1, FOLD)


def shards(init_state, torque, contact, mass_inverse, *vectors):
    core = lax.axis_index("c").astype(jnp.int32)
    chip = (lax.axis_index("x") * lax.axis_size("z") + lax.axis_index("z")).astype(jnp.int32)

    mass_back = swapped(mass_inverse)
    torque = torque.transpose(1, 0, 2)
    counts = local_call(count_kernel, "count", [(8, 4, LANES)], [], core[None], contact)
    send = local_call(split_kernel, "split", [SWAP], [], core[None], torque, contact)
    back = swapped(send)
    counts = lax.all_to_all(counts, ("c", "y"), split_axis=0, concat_axis=0, tiled=True)
    totals = counts.reshape(2, BLOCKS, 4, LANES).sum(axis=1).reshape(8, LANES)
    order = core == 0
    matrices = folded(
        jnp.where(
            order,
            jnp.concatenate([mass_inverse, mass_back]),
            jnp.concatenate([mass_back, mass_inverse]),
        )
    )
    mass_rows = matrices[:, : MASS_ROWS * LANES].reshape(GROUP * MASS_ROWS, LANES)
    mass_tails = matrices[:, MASS_ROWS * LANES :].T

    sent = local_call(
        pack_kernel,
        "pack",
        [(CHIPS, CHUNKS, LANES)],
        [(3 * LANES, LANES)],
        core[None],
        torque,
        contact,
        back,
        totals,
        mass_rows,
        mass_tails,
    )
    sent, place, par, init = lax.optimization_barrier(
        (sent, jnp.stack([chip, core]), param_table(*vectors), init_state)
    )
    solved = main_call(place, init, exchanged(sent), par)
    mine, send = local_call(
        unpack_kernel, "unpack", [SWAP, SWAP], [(3 * LANES, LANES)], core[None], exchanged(solved)
    )
    final, corr = local_call(
        join_kernel, "join", [(2 * DOF, 2, 2 * LANES), (ITERS, 2 * LANES)], [], core[None], mine, swapped(send)
    )
    return final.transpose(1, 0, 2), corr


def solution(mesh):
    torus = Mesh(mesh.devices.reshape(4, 8, 2, mesh.shape["env"]), ("x", "z", "c", "y"))
    return jax.shard_map(
        shards,
        mesh=torus,
        in_specs=(P(None, "y"), P(TM, None, "y"), P(TM, "y"), P(TM, None, None), P(), P(), P(), P(), P()),
        out_specs=(P(TM, None, "y"), P(None, "y")),
        check_vma=False,
    )
```

```python
import functools
import math

import jax
import jax.numpy as jnp
from jax import lax
from jax.experimental import pallas as pl
from jax.experimental.pallas import tpu as pltpu
from jax.sharding import Mesh
from jax.sharding import PartitionSpec as P

DOF = 35
PAD = 40
HS = 2
SUB = 32
ITERS = 3
GROUP = 4
BLOCKS = 4
CHIPS = 32
STEPS = GROUP * HS
LANES = 128
ENV = 1024
TM = ("x", "z", "c")
PEERS = ("x", "z")

DT = 0.05
FINE = DT / SUB
TURN = 1.0 / (2.0 * math.pi)
SINE = tuple(4.0 * c for c in (6.283182595389212, -16.20867027746649, 16.7609745050196, -9.530799181282873, 3.0583252710952205))

ROW_CONTACT = STEPS * PAD
ROW_COUNT = ROW_CONTACT + 8
ROW_TAIL = ROW_COUNT + 8
IN_ROWS = 12
FOLD_ROWS = 18
FOLD_COLS = 36
FOLD = FOLD_ROWS * FOLD_COLS
MASS_ROWS = 5
CHUNKS = IN_ROWS + GROUP * MASS_ROWS
VMEM_LIMIT = 24 * 1024 * 1024
ALL_VMEM = 67_043_328

f32 = jnp.float32


def lane_index(rows):
    return lax.broadcasted_iota(jnp.int32, (rows, LANES), 1)


def block_transpose(parts):
    lane = lane_index(parts[0].shape[0])
    low = lane < 64
    even = ((lane >> 5) & 1) == 0
    a, b, c, d = parts
    a, c = jnp.where(low, a, pltpu.roll(c, 64, 1)), jnp.where(low, pltpu.roll(a, 64, 1), c)
    b, d = jnp.where(low, b, pltpu.roll(d, 64, 1)), jnp.where(low, pltpu.roll(b, 64, 1), d)
    a, b = jnp.where(even, a, pltpu.roll(b, 32, 1)), jnp.where(even, pltpu.roll(a, 96, 1), b)
    c, d = jnp.where(even, c, pltpu.roll(d, 32, 1)), jnp.where(even, pltpu.roll(c, 96, 1), d)
    return a, b, c, d


def block_spread(value):
    block = lane_index(value.shape[0]) >> 5
    turned = [value] + [pltpu.roll(value, 32 * m, 1) for m in (1, 2, 3)]
    return [
        jnp.where(
            block < 2,
            jnp.where(block == 0, turned[(0 - c) % 4], turned[(1 - c) % 4]),
            jnp.where(block == 2, turned[(2 - c) % 4], turned[(3 - c) % 4]),
        )
        for c in range(4)
    ]


def shifted(value, by):
    group = lane_index(value.shape[0]) & 31
    return jnp.where(group >= by, pltpu.roll(value, by, 1), 0.0)


def fold_index(k, i):
    k, i = min(k, i), max(k, i)
    if k < FOLD_ROWS:
        return k * FOLD_COLS + i + 1
    return (DOF - 1 - k) * FOLD_COLS + DOF - 1 - i


def half_of(which):
    return pl.ds(pl.multiple_of(which * LANES, LANES), LANES)


def split_kernel(
    core, contact, torque, mass, v0, v1, v2, v3, v4,
    counts, table, mass_out, own, send,
    contact_in, torque_in, vectors_in, spare, sems,
):
    vectors = (v0, v1, v2, v3, v4)
    pairs = [(contact, contact_in), (torque, torque_in), (mass, mass_out)]
    pairs += [(v, vectors_in.at[i]) for i, v in enumerate(vectors)]
    copies = [pltpu.make_async_copy(a, b, sems.at[i]) for i, (a, b) in enumerate(pairs)]
    for copy in copies:
        copy.start()
    own[...] = jnp.zeros_like(own)
    send[...] = jnp.zeros_like(send)
    spare[...] = jnp.zeros_like(spare)
    copies[0].wait()
    total = jnp.sum(contact_in[...].astype(f32), axis=1, keepdims=True)
    for peer in range(8):
        counts[peer] = jnp.broadcast_to(total, (4, LANES))
    for copy in copies[3:]:
        copy.wait()
    for i in range(len(vectors)):
        spare[i : i + 1, 0:DOF] = vectors_in[i]
    table[...] = spare[...].T[0:PAD, 0:8]
    copies[2].wait()
    copies[1].wait()
    for ref, which in ((own, core[0]), (send, 1 - core[0])):
        part = half_of(which)
        for t in range(4):
            ref[t * PAD : t * PAD + DOF, :] = torque_in[:, t, part]
        ref[4 * PAD : 4 * PAD + 4, :] = contact_in[:, part].astype(f32)


def pack_kernel(core, own, back, totals, mass, tails, out, rows):
    me = core[0]
    rows[...] = jnp.zeros_like(rows)
    for ref, which in ((own, me), (back, 1 - me)):
        rows[pl.ds(pl.multiple_of(which * 4 * PAD, 8), 4 * PAD), :] = ref[0 : 4 * PAD, :]
    own, other = (ref[4 * PAD : 4 * PAD + 4, :] for ref in (own, back))
    rows[ROW_CONTACT : ROW_CONTACT + 8, :] = jnp.where(
        me == 0, jnp.concatenate([own, other]), jnp.concatenate([other, own])
    )
    rows[ROW_COUNT : ROW_COUNT + 8, :] = totals[...]
    block = lane_index(8) >> 5
    tail = jnp.zeros((8, LANES), f32)
    for b in range(GROUP):
        tail = jnp.where(block == b, tails[:, b : b + 1], tail)
    rows[ROW_TAIL : ROW_TAIL + 8, :] = tail
    for c in range(3):
        turned = rows[c * LANES : (c + 1) * LANES, :].T
        for e in range(BLOCKS):
            out[:, e * 3 + c, :] = turned[e * CHIPS : (e + 1) * CHIPS]
    for m in range(GROUP * MASS_ROWS):
        out[:, IN_ROWS + m, :] = jnp.broadcast_to(mass[m : m + 1, :], (CHIPS, LANES))


def state_row(k):
    return k if k < DOF else k + PAD - DOF


def main_kernel(
    chip, init_ref, recv, par, out, rows, fold, mb, ma, wide, cols, tau_b, stiff_b, damp_b, spring, fric, start, end, shift, pos, vel, force, vec, corr
):
    for c in range(3):
        rows[c * LANES : (c + 1) * LANES, :] = jnp.concatenate(
            [recv[:, e * 3 + c, :] for e in range(BLOCKS)]
        ).T
    for m in range(MASS_ROWS):
        fold[m * LANES : (m + 1) * LANES, :] = jnp.concatenate(
            [recv[:, IN_ROWS + b * MASS_ROWS + m, :] for b in range(GROUP)]
        ).T
    fold[MASS_ROWS * LANES : FOLD, :] = rows[ROW_TAIL : ROW_TAIL + 8, :]

    def param(i):
        return jnp.broadcast_to(par[:, i : i + 1], (PAD, LANES))

    stiffness, damping, gravity, contact_stiffness, contact_damping = (param(i) for i in range(5))

    for k in range(DOF):
        for i in range(DOF):
            at = fold_index(k, i)
            mb[k, i : i + 1, :] = fold[at : at + 1, :]
        mb[k, DOF:PAD, :] = jnp.zeros((PAD - DOF, LANES), f32)

    def place_mass(n, carry):
        for k in range(5):
            for b, spread in enumerate(block_spread(mb[5 * n + k])):
                ma[b, 5 * n + k] = spread
        return carry

    lax.fori_loop(0, DOF // 5, place_mass, 0)

    mean = rows[ROW_COUNT : ROW_COUNT + 8, :] / ENV
    for t in range(STEPS):
        here = mean[t : t + 1, :]
        spring[t] = (stiffness + gravity + here * contact_stiffness) * (FINE * DT)
        fric[t] = (damping + here * contact_damping) * DT

    for j in range(HS):
        turned = block_transpose([rows[(2 * b + j) * PAD : (2 * b + j + 1) * PAD, :] for b in range(GROUP)])
        touch = block_transpose(
            [rows[ROW_CONTACT + 2 * b + j : ROW_CONTACT + 2 * b + j + 1, :] for b in range(GROUP)]
        )
        for e in range(BLOCKS):
            tau_b[j, e] = turned[e] * (FINE * FINE * TURN)
            stiff_b[j, e] = (stiffness + touch[e] * contact_stiffness) * (FINE * FINE)
            damp_b[j, e] = (damping + touch[e] * contact_damping) * FINE

    grav = gravity * (FINE * FINE * TURN)

    def half_step(b, t, states, driven):
        moved = []
        for n, (q, w) in enumerate(states):
            pull = spring[t] * q + fric[t] * w
            if driven:
                pull = rows[pl.ds(pl.multiple_of(t * PAD, 8), PAD), :] * (FINE * DT * TURN) - pull
            else:
                pull = -pull
            vec[n, 0:PAD, :] = pull
            moved.append(w)
        for k in range(DOF):
            mass = ma[b, k]
            for n in range(len(states)):
                moved[n] = moved[n] + mass * vec[n, k : k + 1, :]
        return tuple((q + float(SUB) * w, w) for (q, _), w in zip(states, moved))

    def slice_step(b, states, driven):
        return half_step(b, 2 * b + 1, half_step(b, 2 * b, states, driven), driven)

    def one_slice(b, q, w, driven):
        return slice_step(b, ((q, w),), driven)[0]

    def apply_wide(level, row_of):
        low = high = None
        for k in range(2 * DOF):
            row = row_of(state_row(k))
            term = wide[level, k, :PAD, :] * row
            low = term if low is None else low + term
            if k < DOF:
                term = wide[level, k, PAD:, :] * row
                high = term if high is None else high + term
        for k in range(DOF, 2 * DOF):
            high = high + wide[level, k, PAD:, :] * row_of(state_row(k))
        return low, high

    row80 = lax.broadcasted_iota(jnp.int32, (2 * PAD, LANES), 0)
    col_block = lane_index(2 * PAD) >> 5

    def first_half(base, q, w):
        for c in range(4):
            k = base + c
            r = jnp.minimum(jnp.where(k < DOF, k, k - DOF), DOF - 1)
            row = jnp.where(k < DOF, spring[0, pl.ds(r, 1), :], fric[0, pl.ds(r, 1), :])
            w = w - jnp.where(col_block[:PAD] == c, ma[0, r] * row, 0.0)
        return q + float(SUB) * w, w

    def first_columns(pair, carry):
        states = []
        for n in range(2):
            col = 4 * (2 * pair + n) + col_block
            col = jnp.where(col < DOF, col, col + (PAD - DOF))
            unit = jnp.where(row80 == col, 1.0, 0.0)
            states.append(first_half(4 * (2 * pair + n), unit[:PAD], unit[PAD:]))
        states = half_step(0, 1, states, False)
        states = lax.fori_loop(1, GROUP, lambda b, now: slice_step(b, now, False), states)
        for n in range(2):
            cols[2 * pair + n, :PAD, :] = states[n][0]
            cols[2 * pair + n, PAD:, :] = states[n][1]
        return carry

    lax.fori_loop(0, 9, first_columns, 0)

    def spread_columns(level, by):
        def some(n, carry):
            for m in range(3):
                value = cols[3 * n + m]
                for c, spread in enumerate(block_spread(value)):
                    wide[level, 4 * (3 * n + m) + c] = spread
                if by:
                    cols[3 * n + m] = shifted(value, by)
            return carry

        lax.fori_loop(0, 6, some, 0)

    def more_columns(level):
        def one(cg, carry):
            low, high = apply_wide(level - 1, lambda r: cols[cg, r : r + 1, :])
            cols[cg, :PAD, :] = low
            cols[cg, PAD:, :] = high
            return carry

        lax.fori_loop(0, 18, one, 0)

    spread_columns(0, 1)
    more_columns(1)
    spread_columns(1, 2)
    more_columns(2)
    spread_columns(2, 0)

    def scan_groups(q, w):
        def add_earlier(level, by, slot, base, state):
            vec[slot, :PAD, :] = shifted(state[0], by)
            vec[slot, PAD:, :] = shifted(state[1], by)
            low, high = apply_wide(level, lambda r: vec[slot, r : r + 1, :])
            return base[0] + low, base[1] + high

        state = (q, w)
        state = add_earlier(0, 1, 0, state, state)
        state = base = add_earlier(1, 2, 1, state, state)
        for n in range(7):
            state = add_earlier(2, 4, n % 2, base, state)
        return state

    first = (lane_index(2 * PAD) & 31) == 0
    back_by = LANES - chip[0]
    vec[0] = jnp.zeros((2 * PAD, LANES), f32)
    vec[0, 0:DOF, :] = init_ref[:DOF, half_of(chip[1])] * TURN
    vec[0, PAD : PAD + DOF, :] = init_ref[DOF:, half_of(chip[1])] * (FINE * TURN)
    init = jnp.where(first, pltpu.roll(vec[0], back_by, 1), 0.0)

    def driven_slice(b, qw):
        return one_slice(b, qw[0], qw[1], True)

    q, w = lax.fori_loop(0, GROUP, driven_slice, (init[:PAD], init[PAD:]))
    q, w = scan_groups(q, w)
    first = first[:PAD]
    entry = jnp.where(first, init[:PAD], shifted(q, 1)), jnp.where(first, init[PAD:], shifted(w, 1))

    def driven_keep(b, qw):
        start[b, :PAD, :], start[b, PAD:, :] = qw
        qw = one_slice(b, qw[0], qw[1], True)
        end[b, :PAD, :], end[b, PAD:, :] = qw
        return qw

    lax.fori_loop(0, GROUP, driven_keep, entry)

    corr[...] = jnp.zeros_like(corr)

    def iteration(it, carry):
        for half, ref in ((0, pos), (PAD, vel)):
            for e, part in enumerate(block_transpose([start[b, half : half + PAD, :] for b in range(GROUP)])):
                ref[e] = part

        def substep(n, carry):
            j = n // SUB
            for e in range(BLOCKS):
                p = pos[e]
                f = p - jnp.round(p)
                s = f * f
                poly = SINE[4] * s + SINE[3]
                for coef in (SINE[2], SINE[1], SINE[0]):
                    poly = poly * s + coef
                sine = (f * (0.25 - s)) * poly
                force[e] = tau_b[j, e] - stiff_b[j, e] * p - damp_b[j, e] * vel[e] - grav * sine
            acc = [vel[e] for e in range(BLOCKS)]
            for k in range(DOF):
                mass = mb[k]
                for e in range(BLOCKS):
                    acc[e] = acc[e] + mass * force[e, k : k + 1, :]
            for e in range(BLOCKS):
                vel[e] = acc[e]
                pos[e] = pos[e] + acc[e]
            return carry

        lax.fori_loop(0, HS * SUB, substep, 0)
        for half, ref in ((0, pos), (PAD, vel)):
            for b, part in enumerate(block_transpose([ref[e] for e in range(BLOCKS)])):
                shift[b, half : half + PAD, :] = part - end[b, half : half + PAD, :]

        def chain(b, qw):
            q, w = one_slice(b, qw[0], qw[1], False)
            return q + shift[b, :PAD, :], w + shift[b, PAD:, :]

        q, w = lax.fori_loop(1, GROUP, chain, (shift[0, :PAD, :], shift[0, PAD:, :]))
        q, w = scan_groups(q, w)

        def keep(b, state):
            q, w, largest = state
            start[b, :PAD, :] = start[b, :PAD, :] + q
            start[b, PAD:, :] = start[b, PAD:, :] + w
            q, w = chain(b, (q, w))
            end[b, :PAD, :] = end[b, :PAD, :] + q
            end[b, PAD:, :] = end[b, PAD:, :] + w
            dq = q * (1.0 / TURN)
            dv = w * (1.0 / (TURN * FINE))
            square = jnp.sum(dq * dq + dv * dv, axis=0, keepdims=True)
            return q, w, jnp.maximum(largest, square)

        _, _, largest = lax.fori_loop(
            0, GROUP, keep, (shifted(q, 1), shifted(w, 1), jnp.zeros((1, LANES), f32))
        )
        group = lane_index(1) & 31
        for by in (16, 8, 4, 2, 1):
            other = jnp.where(group >= by, pltpu.roll(largest, by, 1), pltpu.roll(largest, LANES - 32 + by, 1))
            largest = jnp.maximum(largest, other)
        corr[pl.ds(it, 1), :] = jnp.sqrt(largest)
        return carry

    lax.fori_loop(0, ITERS, iteration, 0)

    for b in range(GROUP):
        rows[b * 2 * PAD : b * 2 * PAD + PAD, :] = end[b, :PAD, :] * (1.0 / TURN)
        rows[b * 2 * PAD + PAD : (b + 1) * 2 * PAD, :] = end[b, PAD:, :] * (1.0 / (TURN * FINE))
    rows[GROUP * 2 * PAD : GROUP * 2 * PAD + 8, :] = corr[...]
    for c in range(3):
        turned = rows[c * LANES : (c + 1) * LANES, :].T
        for e in range(BLOCKS):
            at = e * 3 + c
            out[:, at // 4, at % 4, :] = turned[e * CHIPS : (e + 1) * CHIPS]


def unpack_kernel(core, recv, mine, send, rows):
    for c in range(3):
        at = [e * 3 + c for e in range(BLOCKS)]
        rows[c * LANES : (c + 1) * LANES, :] = jnp.concatenate([recv[:, i // 4, i % 4, :] for i in at]).T
    corr = rows[GROUP * 2 * PAD : GROUP * 2 * PAD + 8, :]
    for ref, which in ((mine, core[0]), (send, 1 - core[0])):
        ref[0 : 4 * PAD, :] = rows[pl.ds(pl.multiple_of(which * 4 * PAD, 8), 4 * PAD), :]
        ref[4 * PAD :, :] = corr


def join_kernel(core, mine, back, out, corr):
    for ref, which in ((mine, core[0]), (back, 1 - core[0])):
        part = half_of(which)
        for s in range(2):
            out[0:DOF, s, part] = ref[s * 2 * PAD : s * 2 * PAD + DOF, :]
            out[DOF : 2 * DOF, s, part] = ref[s * 2 * PAD + PAD : s * 2 * PAD + PAD + DOF, :]
        corr[:, part] = ref[4 * PAD : 4 * PAD + ITERS, :]


SWAP = (4 * PAD + 8, LANES)


def local_call(kernel, name, out_shapes, scratch, scalars, *arrays):
    smem = pl.BlockSpec(memory_space=pltpu.SMEM)
    vmem = pl.BlockSpec(memory_space=pltpu.VMEM)
    shapes = tuple(jax.ShapeDtypeStruct(shape, f32) for shape in out_shapes)
    return pl.pallas_call(
        kernel,
        in_specs=[smem] + [vmem] * len(arrays),
        out_specs=tuple(vmem for _ in shapes) if len(shapes) > 1 else vmem,
        out_shape=shapes if len(shapes) > 1 else shapes[0],
        scratch_shapes=[pltpu.VMEM(shape, f32) for shape in scratch],
        compiler_params=pltpu.CompilerParams(vmem_limit_bytes=VMEM_LIMIT),
        name=name,
    )(scalars, *arrays)


def main_call(chip, init, recv, par):
    tile = (PAD, LANES)
    scratch = [
        (3 * LANES, LANES),
        (FOLD, LANES),
        (DOF, *tile),
        (GROUP, DOF, *tile),
        (3, 72, 2 * PAD, LANES),
        (18, 2 * PAD, LANES),
        (HS, BLOCKS, *tile),
        (HS, BLOCKS, *tile),
        (HS, BLOCKS, *tile),
        (STEPS, *tile),
        (STEPS, *tile),
        (GROUP, 2 * PAD, LANES),
        (GROUP, 2 * PAD, LANES),
        (GROUP, 2 * PAD, LANES),
        (BLOCKS, *tile),
        (BLOCKS, *tile),
        (BLOCKS, *tile),
        (2, 2 * PAD, LANES),
        (8, LANES),
    ]
    return local_call(main_kernel, "parareal", [(CHIPS, 3, 4, LANES)], scratch, chip, init, recv, par)


def swapped(value):
    return lax.ppermute(value, "c", [(0, 1), (1, 0)])


def exchanged(value):
    return lax.all_to_all(value, PEERS, split_axis=0, concat_axis=0, tiled=True)


def folded(matrices):
    row = lax.broadcasted_iota(jnp.int32, (FOLD_ROWS, FOLD_COLS), 0)
    col = lax.broadcasted_iota(jnp.int32, (FOLD_ROWS, FOLD_COLS), 1)
    plain = jnp.pad(matrices, ((0, 0), (0, 0), (1, 0)))[:, :FOLD_ROWS]
    turned = jnp.pad(matrices[:, ::-1, ::-1], ((0, 0), (0, 0), (0, 1)))[:, :FOLD_ROWS]
    return jnp.where(col <= row, turned, plain).reshape(-1, FOLD)


def shards(init_state, torque, contact, mass_inverse, *vectors):
    core = lax.axis_index("c").astype(jnp.int32)
    chip = (lax.axis_index("x") * lax.axis_size("z") + lax.axis_index("z")).astype(jnp.int32)

    smem = pl.BlockSpec(memory_space=pltpu.SMEM)
    hbm = pl.BlockSpec(memory_space=pltpu.HBM)
    vmem = pl.BlockSpec(memory_space=pltpu.VMEM)
    steps, dof = torque.shape[:2]
    shapes = [(8, 4, LANES), (PAD, 8), (dof, 2, dof), SWAP, SWAP]
    counts, par, mass, own, send = pl.pallas_call(
        split_kernel,
        in_specs=[smem] + [hbm] * 8,
        out_specs=(vmem,) * len(shapes),
        out_shape=tuple(jax.ShapeDtypeStruct(shape, f32) for shape in shapes),
        scratch_shapes=[
            pltpu.VMEM((steps, 2 * LANES), jnp.int32),
            pltpu.VMEM((dof, steps, 2 * LANES), f32),
            pltpu.VMEM((5, 1, dof), f32),
            pltpu.VMEM((LANES, LANES), f32),
            pltpu.SemaphoreType.DMA((8,)),
        ],
        compiler_params=pltpu.CompilerParams(vmem_limit_bytes=ALL_VMEM),
        name="split",
    )(
        core[None],
        contact,
        torque.transpose(1, 0, 2),
        mass_inverse.transpose(1, 0, 2),
        *[v[None] for v in vectors],
    )
    back = swapped(send)
    counts = lax.all_to_all(counts, ("c", "y"), split_axis=0, concat_axis=0, tiled=True)
    totals = counts.reshape(2, BLOCKS, 4, LANES).sum(axis=1).reshape(8, LANES)
    order = core == 0
    mass_back = swapped(mass)
    matrices = folded(
        jnp.where(
            order,
            jnp.concatenate([mass, mass_back], axis=1),
            jnp.concatenate([mass_back, mass], axis=1),
        ).transpose(1, 0, 2)
    )
    mass_rows = matrices[:, : MASS_ROWS * LANES].reshape(GROUP * MASS_ROWS, LANES)
    mass_tails = matrices[:, MASS_ROWS * LANES :].T

    sent = local_call(
        pack_kernel,
        "pack",
        [(CHIPS, CHUNKS, LANES)],
        [(3 * LANES, LANES)],
        core[None],
        own,
        back,
        totals,
        mass_rows,
        mass_tails,
    )
    sent, place, par, init = lax.optimization_barrier(
        (sent, jnp.stack([chip, core]), par, init_state)
    )
    solved = main_call(place, init, exchanged(sent), par)
    mine, send = local_call(
        unpack_kernel, "unpack", [SWAP, SWAP], [(3 * LANES, LANES)], core[None], exchanged(solved)
    )
    final, corr = local_call(
        join_kernel, "join", [(2 * DOF, 2, 2 * LANES), (ITERS, 2 * LANES)], [], core[None], mine, swapped(send)
    )
    return final.transpose(1, 0, 2), corr


def solution(mesh):
    torus = Mesh(mesh.devices.reshape(4, 8, 2, mesh.shape["env"]), ("x", "z", "c", "y"))
    return jax.shard_map(
        shards,
        mesh=torus,
        in_specs=(P(None, "y"), P(TM, None, "y"), P(TM, "y"), P(TM, None, None), P(), P(), P(), P(), P()),
        out_specs=(P(TM, None, "y"), P(None, "y")),
        check_vma=False,
    )
```

```python
import functools
import math

import jax
import jax.numpy as jnp
from jax import lax
from jax.experimental import pallas as pl
from jax.experimental.pallas import tpu as pltpu
from jax.sharding import Mesh
from jax.sharding import PartitionSpec as P

DOF = 35
PAD = 40
HS = 2
SUB = 32
ITERS = 3
GROUP = 4
BLOCKS = 4
CHIPS = 32
STEPS = GROUP * HS
LANES = 128
ENV = 1024
MAIN = 32
DENSE = BLOCKS * MAIN + 16
TM = ("x", "z", "c")
PEERS = ("x", "z")

DT = 0.05
FINE = DT / SUB
TURN = 1.0 / (2.0 * math.pi)
SINE = tuple(4.0 * c for c in (6.283182595389212, -16.20867027746649, 16.7609745050196, -9.530799181282873, 3.0583252710952205))

ROW_CONTACT = STEPS * PAD
ROW_COUNT = ROW_CONTACT + 8
ROW_TAIL = ROW_COUNT + 8
IN_ROWS = 12
FOLD_ROWS = 18
FOLD_COLS = 36
FOLD = FOLD_ROWS * FOLD_COLS
MASS_ROWS = 5
CHUNKS = IN_ROWS + GROUP * MASS_ROWS
VMEM_LIMIT = 24 * 1024 * 1024
ALL_VMEM = 67_043_328

f32 = jnp.float32


def lane_index(rows):
    return lax.broadcasted_iota(jnp.int32, (rows, LANES), 1)


def block_transpose(parts):
    lane = lane_index(parts[0].shape[0])
    low = lane < 64
    even = ((lane >> 5) & 1) == 0
    a, b, c, d = parts
    a, c = jnp.where(low, a, pltpu.roll(c, 64, 1)), jnp.where(low, pltpu.roll(a, 64, 1), c)
    b, d = jnp.where(low, b, pltpu.roll(d, 64, 1)), jnp.where(low, pltpu.roll(b, 64, 1), d)
    a, b = jnp.where(even, a, pltpu.roll(b, 32, 1)), jnp.where(even, pltpu.roll(a, 96, 1), b)
    c, d = jnp.where(even, c, pltpu.roll(d, 32, 1)), jnp.where(even, pltpu.roll(c, 96, 1), d)
    return a, b, c, d


def block_spread(value):
    block = lane_index(value.shape[0]) >> 5
    turned = [value] + [pltpu.roll(value, 32 * m, 1) for m in (1, 2, 3)]
    return [
        jnp.where(
            block < 2,
            jnp.where(block == 0, turned[(0 - c) % 4], turned[(1 - c) % 4]),
            jnp.where(block == 2, turned[(2 - c) % 4], turned[(3 - c) % 4]),
        )
        for c in range(4)
    ]


def fine_row(e, i):
    return e * MAIN + i if i < MAIN else BLOCKS * MAIN + 4 * e + i - MAIN


def put_fine(ref, e, part):
    ref[e * MAIN : (e + 1) * MAIN, :] = part[:MAIN]
    ref[fine_row(e, MAIN) : fine_row(e, MAIN) + DOF - MAIN, :] = part[MAIN:DOF]


def get_fine(ref, e):
    tail = ref[fine_row(e, MAIN) : fine_row(e, MAIN) + DOF - MAIN, :]
    return jnp.concatenate([ref[e * MAIN : (e + 1) * MAIN, :], tail])


def shifted(value, by):
    group = lane_index(value.shape[0]) & 31
    return jnp.where(group >= by, pltpu.roll(value, by, 1), 0.0)


def fold_index(k, i):
    k, i = min(k, i), max(k, i)
    if k < FOLD_ROWS:
        return k * FOLD_COLS + i + 1
    return (DOF - 1 - k) * FOLD_COLS + DOF - 1 - i


def half_of(which):
    return pl.ds(pl.multiple_of(which * LANES, LANES), LANES)


def split_kernel(
    core, contact, torque, mass, v0, v1, v2, v3, v4,
    counts, table, mass_out, own, send,
    contact_in, torque_in, vectors_in, spare, sems,
):
    vectors = (v0, v1, v2, v3, v4)
    pairs = [(contact, contact_in), (torque, torque_in), (mass, mass_out)]
    pairs += [(v, vectors_in.at[i]) for i, v in enumerate(vectors)]
    copies = [pltpu.make_async_copy(a, b, sems.at[i]) for i, (a, b) in enumerate(pairs)]
    for copy in copies:
        copy.start()
    own[...] = jnp.zeros_like(own)
    send[...] = jnp.zeros_like(send)
    spare[...] = jnp.zeros_like(spare)
    copies[0].wait()
    total = jnp.sum(contact_in[...].astype(f32), axis=1, keepdims=True)
    for peer in range(8):
        counts[peer] = jnp.broadcast_to(total, (4, LANES))
    for copy in copies[3:]:
        copy.wait()
    for i in range(len(vectors)):
        spare[i : i + 1, 0:DOF] = vectors_in[i]
    table[...] = spare[...].T[0:PAD, 0:8]
    copies[2].wait()
    copies[1].wait()
    for ref, which in ((own, core[0]), (send, 1 - core[0])):
        part = half_of(which)
        for t in range(4):
            ref[t * PAD : t * PAD + DOF, :] = torque_in[:, t, part]
        ref[4 * PAD : 4 * PAD + 4, :] = contact_in[:, part].astype(f32)


def pack_kernel(core, own, back, totals, mass, tails, out, rows):
    me = core[0]
    rows[...] = jnp.zeros_like(rows)
    for ref, which in ((own, me), (back, 1 - me)):
        rows[pl.ds(pl.multiple_of(which * 4 * PAD, 8), 4 * PAD), :] = ref[0 : 4 * PAD, :]
    own, other = (ref[4 * PAD : 4 * PAD + 4, :] for ref in (own, back))
    rows[ROW_CONTACT : ROW_CONTACT + 8, :] = jnp.where(
        me == 0, jnp.concatenate([own, other]), jnp.concatenate([other, own])
    )
    rows[ROW_COUNT : ROW_COUNT + 8, :] = totals[...]
    block = lane_index(8) >> 5
    tail = jnp.zeros((8, LANES), f32)
    for b in range(GROUP):
        tail = jnp.where(block == b, tails[:, b : b + 1], tail)
    rows[ROW_TAIL : ROW_TAIL + 8, :] = tail
    for c in range(3):
        turned = rows[c * LANES : (c + 1) * LANES, :].T
        for e in range(BLOCKS):
            out[:, e * 3 + c, :] = turned[e * CHIPS : (e + 1) * CHIPS]
    for m in range(GROUP * MASS_ROWS):
        out[:, IN_ROWS + m, :] = jnp.broadcast_to(mass[m : m + 1, :], (CHIPS, LANES))


def state_row(k):
    return k if k < DOF else k + PAD - DOF


def main_kernel(
    chip, init_ref, recv, par, out, rows, fold, mb, ma, mx, wide, cols, tau_b, stiff_b, damp_b, grav, spring, fric, start, end, shift, pos, vel, force, vec, corr
):
    for c in range(3):
        rows[c * LANES : (c + 1) * LANES, :] = jnp.concatenate(
            [recv[:, e * 3 + c, :] for e in range(BLOCKS)]
        ).T
    for m in range(MASS_ROWS):
        fold[m * LANES : (m + 1) * LANES, :] = jnp.concatenate(
            [recv[:, IN_ROWS + b * MASS_ROWS + m, :] for b in range(GROUP)]
        ).T
    fold[MASS_ROWS * LANES : FOLD, :] = rows[ROW_TAIL : ROW_TAIL + 8, :]

    def param(i):
        return jnp.broadcast_to(par[:, i : i + 1], (PAD, LANES))

    stiffness, damping, gravity, contact_stiffness, contact_damping = (param(i) for i in range(5))

    for k in range(DOF):
        for i in range(DOF):
            at = fold_index(k, i)
            mb[k, i : i + 1, :] = fold[at : at + 1, :]
        mb[k, DOF:PAD, :] = jnp.zeros((PAD - DOF, LANES), f32)

    def place_mass(n, carry):
        for k in range(5):
            mx[5 * n + k] = jnp.zeros((8, LANES), f32)
            for half in (0, 4):
                mx[5 * n + k, half : half + DOF - MAIN, :] = mb[5 * n + k, MAIN:DOF, :]
            for b, spread in enumerate(block_spread(mb[5 * n + k])):
                ma[b, 5 * n + k] = spread
        return carry

    lax.fori_loop(0, DOF // 5, place_mass, 0)

    mean = rows[ROW_COUNT : ROW_COUNT + 8, :] / ENV
    for t in range(STEPS):
        here = mean[t : t + 1, :]
        spring[t] = (stiffness + gravity + here * contact_stiffness) * (FINE * DT)
        fric[t] = (damping + here * contact_damping) * DT

    for ref in (tau_b, stiff_b, damp_b, grav, shift, pos, vel):
        ref[...] = jnp.zeros_like(ref)
    for j in range(HS):
        turned = block_transpose([rows[(2 * b + j) * PAD : (2 * b + j + 1) * PAD, :] for b in range(GROUP)])
        touch = block_transpose(
            [rows[ROW_CONTACT + 2 * b + j : ROW_CONTACT + 2 * b + j + 1, :] for b in range(GROUP)]
        )
        for e in range(BLOCKS):
            put_fine(tau_b.at[j], e, turned[e] * (FINE * FINE * TURN))
            put_fine(stiff_b.at[j], e, (stiffness + touch[e] * contact_stiffness) * (FINE * FINE))
            put_fine(damp_b.at[j], e, (damping + touch[e] * contact_damping) * FINE)
            put_fine(grav, e, gravity * (FINE * FINE * TURN))

    def half_step(b, t, states, driven):
        moved = []
        for n, (q, w) in enumerate(states):
            pull = spring[t] * q + fric[t] * w
            if driven:
                pull = rows[pl.ds(pl.multiple_of(t * PAD, 8), PAD), :] * (FINE * DT * TURN) - pull
            else:
                pull = -pull
            vec[n, 0:PAD, :] = pull
            moved.append(w)
        for k in range(DOF):
            mass = ma[b, k]
            for n in range(len(states)):
                moved[n] = moved[n] + mass * vec[n, k : k + 1, :]
        return tuple((q + float(SUB) * w, w) for (q, _), w in zip(states, moved))

    def slice_step(b, states, driven):
        return half_step(b, 2 * b + 1, half_step(b, 2 * b, states, driven), driven)

    def one_slice(b, q, w, driven):
        return slice_step(b, ((q, w),), driven)[0]

    def apply_wide(level, row_of):
        low = high = None
        for k in range(2 * DOF):
            row = row_of(state_row(k))
            term = wide[level, k, :PAD, :] * row
            low = term if low is None else low + term
            if k < DOF:
                term = wide[level, k, PAD:, :] * row
                high = term if high is None else high + term
        for k in range(DOF, 2 * DOF):
            high = high + wide[level, k, PAD:, :] * row_of(state_row(k))
        return low, high

    row80 = lax.broadcasted_iota(jnp.int32, (2 * PAD, LANES), 0)
    col_block = lane_index(2 * PAD) >> 5

    def first_half(base, q, w):
        for c in range(4):
            k = base + c
            r = jnp.minimum(jnp.where(k < DOF, k, k - DOF), DOF - 1)
            row = jnp.where(k < DOF, spring[0, pl.ds(r, 1), :], fric[0, pl.ds(r, 1), :])
            w = w - jnp.where(col_block[:PAD] == c, ma[0, r] * row, 0.0)
        return q + float(SUB) * w, w

    def first_columns(pair, carry):
        states = []
        for n in range(2):
            col = 4 * (2 * pair + n) + col_block
            col = jnp.where(col < DOF, col, col + (PAD - DOF))
            unit = jnp.where(row80 == col, 1.0, 0.0)
            states.append(first_half(4 * (2 * pair + n), unit[:PAD], unit[PAD:]))
        states = half_step(0, 1, states, False)
        states = lax.fori_loop(1, GROUP, lambda b, now: slice_step(b, now, False), states)
        for n in range(2):
            cols[2 * pair + n, :PAD, :] = states[n][0]
            cols[2 * pair + n, PAD:, :] = states[n][1]
        return carry

    lax.fori_loop(0, 9, first_columns, 0)

    def spread_columns(level, by):
        def some(n, carry):
            for m in range(3):
                value = cols[3 * n + m]
                for c, spread in enumerate(block_spread(value)):
                    wide[level, 4 * (3 * n + m) + c] = spread
                if by:
                    cols[3 * n + m] = shifted(value, by)
            return carry

        lax.fori_loop(0, 6, some, 0)

    def more_columns(level):
        def two(pair, carry):
            totals = [None] * 4
            for k in range(2 * DOF):
                at = state_row(k)
                parts = (wide[level - 1, k, :PAD, :], wide[level - 1, k, PAD:, :])
                for n in range(2):
                    row = cols[2 * pair + n, at : at + 1, :]
                    for h in range(2):
                        term = parts[h] * row
                        totals[2 * n + h] = term if k == 0 else totals[2 * n + h] + term
            for n in range(2):
                cols[2 * pair + n, :PAD, :] = totals[2 * n]
                cols[2 * pair + n, PAD:, :] = totals[2 * n + 1]
            return carry

        lax.fori_loop(0, 9, two, 0)

    spread_columns(0, 1)
    more_columns(1)
    spread_columns(1, 2)
    more_columns(2)
    spread_columns(2, 0)

    def scan_groups(q, w):
        def add_earlier(level, by, slot, base, state):
            vec[slot, :PAD, :] = shifted(state[0], by)
            vec[slot, PAD:, :] = shifted(state[1], by)
            low, high = apply_wide(level, lambda r: vec[slot, r : r + 1, :])
            return base[0] + low, base[1] + high

        state = (q, w)
        state = add_earlier(0, 1, 0, state, state)
        state = base = add_earlier(1, 2, 1, state, state)
        for n in range(7):
            state = add_earlier(2, 4, n % 2, base, state)
        return state

    first = (lane_index(2 * PAD) & 31) == 0
    back_by = LANES - chip[0]
    vec[0] = jnp.zeros((2 * PAD, LANES), f32)
    vec[0, 0:DOF, :] = init_ref[:DOF, half_of(chip[1])] * TURN
    vec[0, PAD : PAD + DOF, :] = init_ref[DOF:, half_of(chip[1])] * (FINE * TURN)
    init = jnp.where(first, pltpu.roll(vec[0], back_by, 1), 0.0)

    def driven_slice(b, qw):
        return one_slice(b, qw[0], qw[1], True)

    q, w = lax.fori_loop(0, GROUP, driven_slice, (init[:PAD], init[PAD:]))
    q, w = scan_groups(q, w)
    first = first[:PAD]
    entry = jnp.where(first, init[:PAD], shifted(q, 1)), jnp.where(first, init[PAD:], shifted(w, 1))

    def driven_keep(b, qw):
        start[b, :PAD, :], start[b, PAD:, :] = qw
        qw = one_slice(b, qw[0], qw[1], True)
        end[b, :PAD, :], end[b, PAD:, :] = qw
        return qw

    lax.fori_loop(0, GROUP, driven_keep, entry)

    corr[...] = jnp.zeros_like(corr)
    upper = lax.broadcasted_iota(jnp.int32, (8, LANES), 0) < 4

    def iteration(it, carry):
        for half, ref in ((0, pos), (PAD, vel)):
            for e, part in enumerate(block_transpose([start[b, half : half + DOF, :] for b in range(GROUP)])):
                put_fine(ref, e, part)

        def substep(n, carry):
            for u in range(4):
                substep_one(n * 4 + u)
            return carry

        def substep_one(n):
            j = n // SUB
            for v in range(DENSE // 8):
                at = slice(8 * v, 8 * v + 8)
                p = pos[at, :]
                f = p - jnp.round(p)
                s = f * f
                poly = SINE[4] * s + SINE[3]
                for coef in (SINE[2], SINE[1], SINE[0]):
                    poly = poly * s + coef
                sine = (f * (0.25 - s)) * poly
                pull = tau_b[j, at, :] - stiff_b[j, at, :] * p - damp_b[j, at, :] * vel[at, :] - grav[at, :] * sine
                force[at, :] = pull
            acc = [vel[e * MAIN : (e + 1) * MAIN, :] for e in range(BLOCKS)]
            tail = [vel[BLOCKS * MAIN + 8 * n : BLOCKS * MAIN + 8 * n + 8, :] for n in range(2)]
            for k in range(DOF):
                mass = mb[k, :MAIN, :]
                rest = mx[k]
                row = [force[fine_row(e, k) : fine_row(e, k) + 1, :] for e in range(BLOCKS)]
                for e in range(BLOCKS):
                    acc[e] = acc[e] + mass * row[e]
                for n in range(2):
                    tail[n] = tail[n] + rest * jnp.where(upper, row[2 * n], row[2 * n + 1])
            now = jnp.concatenate(acc + tail)
            vel[...] = now
            pos[...] = pos[...] + now

        lax.fori_loop(0, HS * SUB // 4, substep, 0)
        for half, ref in ((0, pos), (PAD, vel)):
            for b, part in enumerate(block_transpose([get_fine(ref, e) for e in range(BLOCKS)])):
                shift[b, half : half + DOF, :] = part - end[b, half : half + DOF, :]

        def chain(b, qw):
            q, w = one_slice(b, qw[0], qw[1], False)
            return q + shift[b, :PAD, :], w + shift[b, PAD:, :]

        q, w = lax.fori_loop(1, GROUP, chain, (shift[0, :PAD, :], shift[0, PAD:, :]))
        q, w = scan_groups(q, w)

        def keep(b, state):
            q, w, largest = state
            start[b, :PAD, :] = start[b, :PAD, :] + q
            start[b, PAD:, :] = start[b, PAD:, :] + w
            q, w = chain(b, (q, w))
            end[b, :PAD, :] = end[b, :PAD, :] + q
            end[b, PAD:, :] = end[b, PAD:, :] + w
            dq = q * (1.0 / TURN)
            dv = w * (1.0 / (TURN * FINE))
            square = jnp.sum(dq * dq + dv * dv, axis=0, keepdims=True)
            return q, w, jnp.maximum(largest, square)

        _, _, largest = lax.fori_loop(
            0, GROUP, keep, (shifted(q, 1), shifted(w, 1), jnp.zeros((1, LANES), f32))
        )
        group = lane_index(1) & 31
        for by in (16, 8, 4, 2, 1):
            other = jnp.where(group >= by, pltpu.roll(largest, by, 1), pltpu.roll(largest, LANES - 32 + by, 1))
            largest = jnp.maximum(largest, other)
        corr[pl.ds(it, 1), :] = jnp.sqrt(largest)
        return carry

    lax.fori_loop(0, ITERS, iteration, 0)

    for b in range(GROUP):
        rows[b * 2 * PAD : b * 2 * PAD + PAD, :] = end[b, :PAD, :] * (1.0 / TURN)
        rows[b * 2 * PAD + PAD : (b + 1) * 2 * PAD, :] = end[b, PAD:, :] * (1.0 / (TURN * FINE))
    rows[GROUP * 2 * PAD : GROUP * 2 * PAD + 8, :] = corr[...]
    for c in range(3):
        turned = rows[c * LANES : (c + 1) * LANES, :].T
        for e in range(BLOCKS):
            at = e * 3 + c
            out[:, at // 4, at % 4, :] = turned[e * CHIPS : (e + 1) * CHIPS]


def unpack_kernel(core, recv, mine, send, rows):
    for c in range(3):
        at = [e * 3 + c for e in range(BLOCKS)]
        rows[c * LANES : (c + 1) * LANES, :] = jnp.concatenate([recv[:, i // 4, i % 4, :] for i in at]).T
    corr = rows[GROUP * 2 * PAD : GROUP * 2 * PAD + 8, :]
    for ref, which in ((mine, core[0]), (send, 1 - core[0])):
        ref[0 : 4 * PAD, :] = rows[pl.ds(pl.multiple_of(which * 4 * PAD, 8), 4 * PAD), :]
        ref[4 * PAD :, :] = corr


def join_kernel(core, mine, back, out, corr):
    for ref, which in ((mine, core[0]), (back, 1 - core[0])):
        part = half_of(which)
        for s in range(2):
            out[0:DOF, s, part] = ref[s * 2 * PAD : s * 2 * PAD + DOF, :]
            out[DOF : 2 * DOF, s, part] = ref[s * 2 * PAD + PAD : s * 2 * PAD + PAD + DOF, :]
        corr[:, part] = ref[4 * PAD : 4 * PAD + ITERS, :]


SWAP = (4 * PAD + 8, LANES)


def local_call(kernel, name, out_shapes, scratch, scalars, *arrays):
    smem = pl.BlockSpec(memory_space=pltpu.SMEM)
    vmem = pl.BlockSpec(memory_space=pltpu.VMEM)
    shapes = tuple(jax.ShapeDtypeStruct(shape, f32) for shape in out_shapes)
    return pl.pallas_call(
        kernel,
        in_specs=[smem] + [vmem] * len(arrays),
        out_specs=tuple(vmem for _ in shapes) if len(shapes) > 1 else vmem,
        out_shape=shapes if len(shapes) > 1 else shapes[0],
        scratch_shapes=[pltpu.VMEM(shape, f32) for shape in scratch],
        compiler_params=pltpu.CompilerParams(vmem_limit_bytes=VMEM_LIMIT),
        name=name,
    )(scalars, *arrays)


def main_call(chip, init, recv, par):
    tile = (PAD, LANES)
    scratch = [
        (3 * LANES, LANES),
        (FOLD, LANES),
        (DOF, *tile),
        (GROUP, DOF, *tile),
        (DOF, 8, LANES),
        (3, 72, 2 * PAD, LANES),
        (18, 2 * PAD, LANES),
        (HS, DENSE, LANES),
        (HS, DENSE, LANES),
        (HS, DENSE, LANES),
        (DENSE, LANES),
        (STEPS, *tile),
        (STEPS, *tile),
        (GROUP, 2 * PAD, LANES),
        (GROUP, 2 * PAD, LANES),
        (GROUP, 2 * PAD, LANES),
        (DENSE, LANES),
        (DENSE, LANES),
        (DENSE, LANES),
        (2, 2 * PAD, LANES),
        (8, LANES),
    ]
    return local_call(main_kernel, "parareal", [(CHIPS, 3, 4, LANES)], scratch, chip, init, recv, par)


def swapped(value):
    return lax.ppermute(value, "c", [(0, 1), (1, 0)])


def exchanged(value):
    return lax.all_to_all(value, PEERS, split_axis=0, concat_axis=0, tiled=True)


def folded(matrices):
    row = lax.broadcasted_iota(jnp.int32, (FOLD_ROWS, FOLD_COLS), 0)
    col = lax.broadcasted_iota(jnp.int32, (FOLD_ROWS, FOLD_COLS), 1)
    plain = jnp.pad(matrices, ((0, 0), (0, 0), (1, 0)))[:, :FOLD_ROWS]
    turned = jnp.pad(matrices[:, ::-1, ::-1], ((0, 0), (0, 0), (0, 1)))[:, :FOLD_ROWS]
    return jnp.where(col <= row, turned, plain).reshape(-1, FOLD)


def shards(init_state, torque, contact, mass_inverse, *vectors):
    core = lax.axis_index("c").astype(jnp.int32)
    chip = (lax.axis_index("x") * lax.axis_size("z") + lax.axis_index("z")).astype(jnp.int32)

    smem = pl.BlockSpec(memory_space=pltpu.SMEM)
    hbm = pl.BlockSpec(memory_space=pltpu.HBM)
    vmem = pl.BlockSpec(memory_space=pltpu.VMEM)
    steps, dof = torque.shape[:2]
    shapes = [(8, 4, LANES), (PAD, 8), (dof, 2, dof), SWAP, SWAP]
    counts, par, mass, own, send = pl.pallas_call(
        split_kernel,
        in_specs=[smem] + [hbm] * 8,
        out_specs=(vmem,) * len(shapes),
        out_shape=tuple(jax.ShapeDtypeStruct(shape, f32) for shape in shapes),
        scratch_shapes=[
            pltpu.VMEM((steps, 2 * LANES), jnp.int32),
            pltpu.VMEM((dof, steps, 2 * LANES), f32),
            pltpu.VMEM((5, 1, dof), f32),
            pltpu.VMEM((LANES, LANES), f32),
            pltpu.SemaphoreType.DMA((8,)),
        ],
        compiler_params=pltpu.CompilerParams(vmem_limit_bytes=ALL_VMEM),
        name="split",
    )(
        core[None],
        contact,
        torque.transpose(1, 0, 2),
        mass_inverse.transpose(1, 0, 2),
        *[v[None] for v in vectors],
    )
    back = swapped(send)
    counts = lax.all_to_all(counts, ("c", "y"), split_axis=0, concat_axis=0, tiled=True)
    totals = counts.reshape(2, BLOCKS, 4, LANES).sum(axis=1).reshape(8, LANES)
    order = core == 0
    mass_back = swapped(mass)
    matrices = folded(
        jnp.where(
            order,
            jnp.concatenate([mass, mass_back], axis=1),
            jnp.concatenate([mass_back, mass], axis=1),
        ).transpose(1, 0, 2)
    )
    mass_rows = matrices[:, : MASS_ROWS * LANES].reshape(GROUP * MASS_ROWS, LANES)
    mass_tails = matrices[:, MASS_ROWS * LANES :].T

    sent = local_call(
        pack_kernel,
        "pack",
        [(CHIPS, CHUNKS, LANES)],
        [(3 * LANES, LANES)],
        core[None],
        own,
        back,
        totals,
        mass_rows,
        mass_tails,
    )
    sent, place, par, init = lax.optimization_barrier(
        (sent, jnp.stack([chip, core]), par, init_state)
    )
    solved = main_call(place, init, exchanged(sent), par)
    mine, send = local_call(
        unpack_kernel, "unpack", [SWAP, SWAP], [(3 * LANES, LANES)], core[None], exchanged(solved)
    )
    final, corr = local_call(
        join_kernel, "join", [(2 * DOF, 2, 2 * LANES), (ITERS, 2 * LANES)], [], core[None], mine, swapped(send)
    )
    return final.transpose(1, 0, 2), corr


def solution(mesh):
    torus = Mesh(mesh.devices.reshape(4, 8, 2, mesh.shape["env"]), ("x", "z", "c", "y"))
    return jax.shard_map(
        shards,
        mesh=torus,
        in_specs=(P(None, "y"), P(TM, None, "y"), P(TM, "y"), P(TM, None, None), P(), P(), P(), P(), P()),
        out_specs=(P(TM, None, "y"), P(None, "y")),
        check_vma=False,
    )
```

```python
import functools
import math

import jax
import jax.numpy as jnp
from jax import lax
from jax.experimental import pallas as pl
from jax.experimental.pallas import tpu as pltpu
from jax.sharding import Mesh
from jax.sharding import PartitionSpec as P

DOF = 35
PAD = 40
HS = 2
SUB = 32
ITERS = 3
GROUP = 4
BLOCKS = 4
CHIPS = 32
STEPS = GROUP * HS
LANES = 128
ENV = 1024
MAIN = 32
DENSE = BLOCKS * MAIN + 16
STATE = 2 * DOF
ROWS = 72
TM = ("x", "z", "c")
PEERS = ("x", "z")

DT = 0.05
FINE = DT / SUB
TURN = 1.0 / (2.0 * math.pi)
SINE = tuple(4.0 * c for c in (6.283182595389212, -16.20867027746649, 16.7609745050196, -9.530799181282873, 3.0583252710952205))

ROW_CONTACT = STEPS * PAD
ROW_COUNT = ROW_CONTACT + 8
ROW_TAIL = ROW_COUNT + 8
IN_ROWS = 12
FOLD_ROWS = 18
FOLD_COLS = 36
FOLD = FOLD_ROWS * FOLD_COLS
MASS_ROWS = 5
CHUNKS = IN_ROWS + GROUP * MASS_ROWS
VMEM_LIMIT = 24 * 1024 * 1024
ALL_VMEM = 67_043_328

f32 = jnp.float32


def lane_index(rows):
    return lax.broadcasted_iota(jnp.int32, (rows, LANES), 1)


def block_transpose(parts):
    lane = lane_index(parts[0].shape[0])
    low = lane < 64
    even = ((lane >> 5) & 1) == 0
    a, b, c, d = parts
    a, c = jnp.where(low, a, pltpu.roll(c, 64, 1)), jnp.where(low, pltpu.roll(a, 64, 1), c)
    b, d = jnp.where(low, b, pltpu.roll(d, 64, 1)), jnp.where(low, pltpu.roll(b, 64, 1), d)
    a, b = jnp.where(even, a, pltpu.roll(b, 32, 1)), jnp.where(even, pltpu.roll(a, 96, 1), b)
    c, d = jnp.where(even, c, pltpu.roll(d, 32, 1)), jnp.where(even, pltpu.roll(c, 96, 1), d)
    return a, b, c, d


def block_spread(value):
    block = lane_index(value.shape[0]) >> 5
    turned = [value] + [pltpu.roll(value, 32 * m, 1) for m in (1, 2, 3)]
    return [
        jnp.where(
            block < 2,
            jnp.where(block == 0, turned[(0 - c) % 4], turned[(1 - c) % 4]),
            jnp.where(block == 2, turned[(2 - c) % 4], turned[(3 - c) % 4]),
        )
        for c in range(4)
    ]


def fine_row(e, i):
    return e * MAIN + i if i < MAIN else BLOCKS * MAIN + 4 * e + i - MAIN


def put_fine(ref, e, part):
    ref[e * MAIN : (e + 1) * MAIN, :] = part[:MAIN]
    ref[fine_row(e, MAIN) : fine_row(e, MAIN) + DOF - MAIN, :] = part[MAIN:DOF]


def get_fine(ref, e):
    tail = ref[fine_row(e, MAIN) : fine_row(e, MAIN) + DOF - MAIN, :]
    return jnp.concatenate([ref[e * MAIN : (e + 1) * MAIN, :], tail])


def shifted(value, by):
    group = lane_index(value.shape[0]) & 31
    return jnp.where(group >= by, pltpu.roll(value, by, 1), 0.0)


def fold_index(k, i):
    k, i = min(k, i), max(k, i)
    if k < FOLD_ROWS:
        return k * FOLD_COLS + i + 1
    return (DOF - 1 - k) * FOLD_COLS + DOF - 1 - i


def half_of(which):
    return pl.ds(pl.multiple_of(which * LANES, LANES), LANES)


def split_kernel(
    core, contact, torque, mass, v0, v1, v2, v3, v4,
    counts, table, mass_out, own, send,
    contact_in, torque_in, vectors_in, spare, sems,
):
    vectors = (v0, v1, v2, v3, v4)
    pairs = [(contact, contact_in), (torque, torque_in), (mass, mass_out)]
    pairs += [(v, vectors_in.at[i]) for i, v in enumerate(vectors)]
    copies = [pltpu.make_async_copy(a, b, sems.at[i]) for i, (a, b) in enumerate(pairs)]
    for copy in copies:
        copy.start()
    own[...] = jnp.zeros_like(own)
    send[...] = jnp.zeros_like(send)
    spare[...] = jnp.zeros_like(spare)
    copies[0].wait()
    total = jnp.sum(contact_in[...].astype(f32), axis=1, keepdims=True)
    for peer in range(8):
        counts[peer] = jnp.broadcast_to(total, (4, LANES))
    for copy in copies[3:]:
        copy.wait()
    for i in range(len(vectors)):
        spare[i : i + 1, 0:DOF] = vectors_in[i]
    table[...] = spare[...].T[0:PAD, 0:8]
    copies[2].wait()
    copies[1].wait()
    for ref, which in ((own, core[0]), (send, 1 - core[0])):
        part = half_of(which)
        for t in range(4):
            ref[t * PAD : t * PAD + DOF, :] = torque_in[:, t, part]
        ref[4 * PAD : 4 * PAD + 4, :] = contact_in[:, part].astype(f32)


def pack_kernel(core, own, back, totals, mass, tails, out, rows):
    me = core[0]
    rows[...] = jnp.zeros_like(rows)
    for ref, which in ((own, me), (back, 1 - me)):
        rows[pl.ds(pl.multiple_of(which * 4 * PAD, 8), 4 * PAD), :] = ref[0 : 4 * PAD, :]
    own, other = (ref[4 * PAD : 4 * PAD + 4, :] for ref in (own, back))
    rows[ROW_CONTACT : ROW_CONTACT + 8, :] = jnp.where(
        me == 0, jnp.concatenate([own, other]), jnp.concatenate([other, own])
    )
    rows[ROW_COUNT : ROW_COUNT + 8, :] = totals[...]
    block = lane_index(8) >> 5
    tail = jnp.zeros((8, LANES), f32)
    for b in range(GROUP):
        tail = jnp.where(block == b, tails[:, b : b + 1], tail)
    rows[ROW_TAIL : ROW_TAIL + 8, :] = tail
    for c in range(3):
        turned = rows[c * LANES : (c + 1) * LANES, :].T
        for e in range(BLOCKS):
            out[:, e * 3 + c, :] = turned[e * CHIPS : (e + 1) * CHIPS]
    for m in range(GROUP * MASS_ROWS):
        out[:, IN_ROWS + m, :] = jnp.broadcast_to(mass[m : m + 1, :], (CHIPS, LANES))


def main_kernel(
    chip, init_ref, recv, par, out, rows, fold, mb, ma, mx, wide, cols, tau_b, stiff_b, damp_b, grav, spring, fric, start, end, shift, diff, pos, vel, force, vec, corr
):
    for c in range(3):
        rows[c * LANES : (c + 1) * LANES, :] = jnp.concatenate(
            [recv[:, e * 3 + c, :] for e in range(BLOCKS)]
        ).T
    for m in range(MASS_ROWS):
        fold[m * LANES : (m + 1) * LANES, :] = jnp.concatenate(
            [recv[:, IN_ROWS + b * MASS_ROWS + m, :] for b in range(GROUP)]
        ).T
    fold[MASS_ROWS * LANES : FOLD, :] = rows[ROW_TAIL : ROW_TAIL + 8, :]

    def param(i):
        return jnp.broadcast_to(par[:, i : i + 1], (PAD, LANES))

    stiffness, damping, gravity, contact_stiffness, contact_damping = (param(i) for i in range(5))

    for k in range(DOF):
        for i in range(DOF):
            at = fold_index(k, i)
            mb[k, i : i + 1, :] = fold[at : at + 1, :]
        mb[k, DOF:PAD, :] = jnp.zeros((PAD - DOF, LANES), f32)

    def place_mass(n, carry):
        for k in range(5):
            mx[5 * n + k] = jnp.zeros((8, LANES), f32)
            for half in (0, 4):
                mx[5 * n + k, half : half + DOF - MAIN, :] = mb[5 * n + k, MAIN:DOF, :]
            for b, spread in enumerate(block_spread(mb[5 * n + k])):
                ma[b, 5 * n + k] = spread
        return carry

    lax.fori_loop(0, DOF // 5, place_mass, 0)

    mean = rows[ROW_COUNT : ROW_COUNT + 8, :] / ENV
    for t in range(STEPS):
        here = mean[t : t + 1, :]
        spring[t] = (stiffness + gravity + here * contact_stiffness) * (FINE * DT)
        fric[t] = (damping + here * contact_damping) * DT

    for ref in (tau_b, stiff_b, damp_b, grav, shift, pos, vel):
        ref[...] = jnp.zeros_like(ref)
    for j in range(HS):
        turned = block_transpose([rows[(2 * b + j) * PAD : (2 * b + j + 1) * PAD, :] for b in range(GROUP)])
        touch = block_transpose(
            [rows[ROW_CONTACT + 2 * b + j : ROW_CONTACT + 2 * b + j + 1, :] for b in range(GROUP)]
        )
        for e in range(BLOCKS):
            put_fine(tau_b.at[j], e, turned[e] * (FINE * FINE * TURN))
            put_fine(stiff_b.at[j], e, (stiffness + touch[e] * contact_stiffness) * (FINE * FINE))
            put_fine(damp_b.at[j], e, (damping + touch[e] * contact_damping) * FINE)
            put_fine(grav, e, gravity * (FINE * FINE * TURN))

    def half_step(b, t, states, driven):
        moved = []
        for n, (q, w) in enumerate(states):
            pull = spring[t] * q + fric[t] * w
            if driven:
                pull = rows[pl.ds(pl.multiple_of(t * PAD, 8), PAD), :] * (FINE * DT * TURN) - pull
            else:
                pull = -pull
            vec[n, 0:PAD, :] = pull
            moved.append(w)
        for k in range(DOF):
            mass = ma[b, k]
            for n in range(len(states)):
                moved[n] = moved[n] + mass * vec[n, k : k + 1, :]
        return tuple((q + float(SUB) * w, w) for (q, _), w in zip(states, moved))

    def slice_step(b, states, driven):
        return half_step(b, 2 * b + 1, half_step(b, 2 * b, states, driven), driven)

    def one_slice(b, q, w, driven):
        return slice_step(b, ((q, w),), driven)[0]

    def apply_wide(level, slot):
        low = high = None
        for k in range(STATE):
            row = vec[slot, k : k + 1, :]
            term = wide[level, k, :PAD, :] * row
            low = term if low is None else low + term
            if k < PAD:
                term = wide[level, k, PAD:, :] * row
                high = term if high is None else high + term
        for k in range(PAD, STATE):
            high = high + wide[level, k, PAD:, :] * vec[slot, k : k + 1, :]
        return low, high

    row80 = lax.broadcasted_iota(jnp.int32, (2 * PAD, LANES), 0)
    col_block = lane_index(2 * PAD) >> 5

    def first_half(base, q, w):
        for c in range(4):
            k = base + c
            r = jnp.minimum(jnp.where(k < DOF, k, k - DOF), DOF - 1)
            row = jnp.where(k < DOF, spring[0, pl.ds(r, 1), :], fric[0, pl.ds(r, 1), :])
            w = w - jnp.where(col_block[:PAD] == c, ma[0, r] * row, 0.0)
        return q + float(SUB) * w, w

    def first_columns(pair, carry):
        states = []
        for n in range(2):
            col = 4 * (2 * pair + n) + col_block
            col = jnp.where(col < DOF, col, col + (PAD - DOF))
            unit = jnp.where(row80 == col, 1.0, 0.0)
            states.append(first_half(4 * (2 * pair + n), unit[:PAD], unit[PAD:]))
        states = half_step(0, 1, states, False)
        states = lax.fori_loop(1, GROUP, lambda b, now: slice_step(b, now, False), states)
        for n in range(2):
            cols[2 * pair + n, :DOF, :] = states[n][0][:DOF]
            cols[2 * pair + n, DOF:STATE, :] = states[n][1][:DOF]
            cols[2 * pair + n, STATE:, :] = jnp.zeros((ROWS - STATE, LANES), f32)
        return carry

    lax.fori_loop(0, 9, first_columns, 0)

    def spread_columns(level, by):
        def some(n, carry):
            for m in range(3):
                value = cols[3 * n + m]
                for c, spread in enumerate(block_spread(value)):
                    wide[level, 4 * (3 * n + m) + c] = spread
                if by:
                    cols[3 * n + m] = shifted(value, by)
            return carry

        lax.fori_loop(0, 6, some, 0)

    def more_columns(level):
        def two(pair, carry):
            totals = [None] * 4
            for k in range(STATE):
                parts = (wide[level - 1, k, :PAD, :], wide[level - 1, k, PAD:, :])
                for n in range(2):
                    row = cols[2 * pair + n, k : k + 1, :]
                    for h in range(2):
                        term = parts[h] * row
                        totals[2 * n + h] = term if k == 0 else totals[2 * n + h] + term
            for n in range(2):
                cols[2 * pair + n, :PAD, :] = totals[2 * n]
                cols[2 * pair + n, PAD:, :] = totals[2 * n + 1]
            return carry

        lax.fori_loop(0, 9, two, 0)

    spread_columns(0, 1)
    more_columns(1)
    spread_columns(1, 2)
    more_columns(2)
    spread_columns(2, 0)

    def scan_groups(q, w):
        def add_earlier(level, by, slot, state):
            vec[slot, :PAD, :] = shifted(state[0], by)
            vec[slot, PAD:ROWS, :] = shifted(state[1], by)
            low, high = apply_wide(level, slot)
            return state[0] + low, state[1] + high

        diff[:DOF, :] = q[:DOF]
        diff[DOF:STATE, :] = w[:DOF]
        diff[STATE:, :] = jnp.zeros((2 * PAD - STATE, LANES), f32)
        base = diff[:PAD, :], diff[PAD:ROWS, :]
        base = add_earlier(0, 1, 0, base)
        base = add_earlier(1, 2, 1, base)
        diff[:PAD, :], diff[PAD:ROWS, :] = base
        vec[0, :PAD, :] = shifted(base[0], 4)

        def more(n, now):
            vec[0, PAD:ROWS, :] = shifted(now[1], 4)
            low, high = diff[:PAD, :], diff[PAD:ROWS, :]
            for k in range(PAD):
                row = vec[0, k : k + 1, :]
                low = low + wide[2, k, :PAD, :] * row
                high = high + wide[2, k, PAD:, :] * row
            for k in range(PAD, STATE):
                low = low + wide[2, k, :PAD, :] * vec[0, k : k + 1, :]
            vec[0, :PAD, :] = shifted(low, 4)
            for k in range(PAD, STATE):
                high = high + wide[2, k, PAD:, :] * vec[0, k : k + 1, :]
            return low, high

        diff[:PAD, :], diff[PAD:ROWS, :] = lax.fori_loop(0, 7, more, base)
        used = lax.broadcasted_iota(jnp.int32, (PAD, LANES), 0) < DOF
        return jnp.where(used, diff[:PAD, :], 0.0), jnp.where(used, diff[DOF : DOF + PAD, :], 0.0)

    first = (lane_index(2 * PAD) & 31) == 0
    back_by = LANES - chip[0]
    vec[0] = jnp.zeros((2 * PAD, LANES), f32)
    vec[0, 0:DOF, :] = init_ref[:DOF, half_of(chip[1])] * TURN
    vec[0, PAD : PAD + DOF, :] = init_ref[DOF:, half_of(chip[1])] * (FINE * TURN)
    init = jnp.where(first, pltpu.roll(vec[0], back_by, 1), 0.0)

    def driven_slice(b, qw):
        return one_slice(b, qw[0], qw[1], True)

    q, w = lax.fori_loop(0, GROUP, driven_slice, (init[:PAD], init[PAD:]))
    q, w = scan_groups(q, w)
    first = first[:PAD]
    entry = jnp.where(first, init[:PAD], shifted(q, 1)), jnp.where(first, init[PAD:], shifted(w, 1))

    def driven_keep(b, qw):
        start[b, :PAD, :], start[b, PAD:, :] = qw
        qw = one_slice(b, qw[0], qw[1], True)
        end[b, :PAD, :], end[b, PAD:, :] = qw
        return qw

    lax.fori_loop(0, GROUP, driven_keep, entry)

    corr[...] = jnp.zeros_like(corr)
    upper = lax.broadcasted_iota(jnp.int32, (8, LANES), 0) < 4

    def iteration(it, carry):
        for half, ref in ((0, pos), (PAD, vel)):
            for e, part in enumerate(block_transpose([start[b, half : half + DOF, :] for b in range(GROUP)])):
                put_fine(ref, e, part)

        def substep(n, carry):
            for u in range(4):
                substep_one(n * 4 + u)
            return carry

        def substep_one(n):
            j = n // SUB
            for v in range(DENSE // 8):
                at = slice(8 * v, 8 * v + 8)
                p = pos[at, :]
                f = p - jnp.round(p)
                s = f * f
                poly = SINE[4] * s + SINE[3]
                for coef in (SINE[2], SINE[1], SINE[0]):
                    poly = poly * s + coef
                sine = (f * (0.25 - s)) * poly
                pull = tau_b[j, at, :] - stiff_b[j, at, :] * p - damp_b[j, at, :] * vel[at, :] - grav[at, :] * sine
                force[at, :] = pull
            acc = [vel[e * MAIN : (e + 1) * MAIN, :] for e in range(BLOCKS)]
            tail = [vel[BLOCKS * MAIN + 8 * n : BLOCKS * MAIN + 8 * n + 8, :] for n in range(2)]
            for k in range(DOF):
                mass = mb[k, :MAIN, :]
                rest = mx[k]
                row = [force[fine_row(e, k) : fine_row(e, k) + 1, :] for e in range(BLOCKS)]
                for e in range(BLOCKS):
                    acc[e] = acc[e] + mass * row[e]
                for n in range(2):
                    tail[n] = tail[n] + rest * jnp.where(upper, row[2 * n], row[2 * n + 1])
            now = jnp.concatenate(acc + tail)
            vel[...] = now
            pos[...] = pos[...] + now

        lax.fori_loop(0, HS * SUB // 4, substep, 0)
        for half, ref in ((0, pos), (PAD, vel)):
            for b, part in enumerate(block_transpose([get_fine(ref, e) for e in range(BLOCKS)])):
                shift[b, half : half + DOF, :] = part - end[b, half : half + DOF, :]

        def chain(b, qw):
            q, w = one_slice(b, qw[0], qw[1], False)
            return q + shift[b, :PAD, :], w + shift[b, PAD:, :]

        q, w = lax.fori_loop(1, GROUP, chain, (shift[0, :PAD, :], shift[0, PAD:, :]))
        q, w = scan_groups(q, w)

        def keep(b, state):
            q, w, largest = state
            start[b, :PAD, :] = start[b, :PAD, :] + q
            start[b, PAD:, :] = start[b, PAD:, :] + w
            q, w = chain(b, (q, w))
            end[b, :PAD, :] = end[b, :PAD, :] + q
            end[b, PAD:, :] = end[b, PAD:, :] + w
            dq = q * (1.0 / TURN)
            dv = w * (1.0 / (TURN * FINE))
            square = jnp.sum(dq * dq + dv * dv, axis=0, keepdims=True)
            return q, w, jnp.maximum(largest, square)

        _, _, largest = lax.fori_loop(
            0, GROUP, keep, (shifted(q, 1), shifted(w, 1), jnp.zeros((1, LANES), f32))
        )
        group = lane_index(1) & 31
        for by in (16, 8, 4, 2, 1):
            other = jnp.where(group >= by, pltpu.roll(largest, by, 1), pltpu.roll(largest, LANES - 32 + by, 1))
            largest = jnp.maximum(largest, other)
        corr[pl.ds(it, 1), :] = jnp.sqrt(largest)
        return carry

    lax.fori_loop(0, ITERS, iteration, 0)

    for b in range(GROUP):
        rows[b * 2 * PAD : b * 2 * PAD + PAD, :] = end[b, :PAD, :] * (1.0 / TURN)
        rows[b * 2 * PAD + PAD : (b + 1) * 2 * PAD, :] = end[b, PAD:, :] * (1.0 / (TURN * FINE))
    rows[GROUP * 2 * PAD : GROUP * 2 * PAD + 8, :] = corr[...]
    for c in range(3):
        turned = rows[c * LANES : (c + 1) * LANES, :].T
        for e in range(BLOCKS):
            at = e * 3 + c
            out[:, at // 4, at % 4, :] = turned[e * CHIPS : (e + 1) * CHIPS]


def unpack_kernel(core, recv, mine, send, rows):
    for c in range(3):
        at = [e * 3 + c for e in range(BLOCKS)]
        rows[c * LANES : (c + 1) * LANES, :] = jnp.concatenate([recv[:, i // 4, i % 4, :] for i in at]).T
    corr = rows[GROUP * 2 * PAD : GROUP * 2 * PAD + 8, :]
    for ref, which in ((mine, core[0]), (send, 1 - core[0])):
        ref[0 : 4 * PAD, :] = rows[pl.ds(pl.multiple_of(which * 4 * PAD, 8), 4 * PAD), :]
        ref[4 * PAD :, :] = corr


def join_kernel(core, mine, back, out, corr):
    for ref, which in ((mine, core[0]), (back, 1 - core[0])):
        part = half_of(which)
        for s in range(2):
            out[0:DOF, s, part] = ref[s * 2 * PAD : s * 2 * PAD + DOF, :]
            out[DOF : 2 * DOF, s, part] = ref[s * 2 * PAD + PAD : s * 2 * PAD + PAD + DOF, :]
        corr[:, part] = ref[4 * PAD : 4 * PAD + ITERS, :]


SWAP = (4 * PAD + 8, LANES)


def local_call(kernel, name, out_shapes, scratch, scalars, *arrays):
    smem = pl.BlockSpec(memory_space=pltpu.SMEM)
    vmem = pl.BlockSpec(memory_space=pltpu.VMEM)
    shapes = tuple(jax.ShapeDtypeStruct(shape, f32) for shape in out_shapes)
    return pl.pallas_call(
        kernel,
        in_specs=[smem] + [vmem] * len(arrays),
        out_specs=tuple(vmem for _ in shapes) if len(shapes) > 1 else vmem,
        out_shape=shapes if len(shapes) > 1 else shapes[0],
        scratch_shapes=[pltpu.VMEM(shape, f32) for shape in scratch],
        compiler_params=pltpu.CompilerParams(vmem_limit_bytes=VMEM_LIMIT),
        name=name,
    )(scalars, *arrays)


def main_call(chip, init, recv, par):
    tile = (PAD, LANES)
    scratch = [
        (3 * LANES, LANES),
        (FOLD, LANES),
        (DOF, *tile),
        (GROUP, DOF, *tile),
        (DOF, 8, LANES),
        (3, 72, ROWS, LANES),
        (18, ROWS, LANES),
        (HS, DENSE, LANES),
        (HS, DENSE, LANES),
        (HS, DENSE, LANES),
        (DENSE, LANES),
        (STEPS, *tile),
        (STEPS, *tile),
        (GROUP, 2 * PAD, LANES),
        (GROUP, 2 * PAD, LANES),
        (GROUP, 2 * PAD, LANES),
        (2 * PAD, LANES),
        (DENSE, LANES),
        (DENSE, LANES),
        (DENSE, LANES),
        (2, 2 * PAD, LANES),
        (8, LANES),
    ]
    return local_call(main_kernel, "parareal", [(CHIPS, 3, 4, LANES)], scratch, chip, init, recv, par)


def swapped(value):
    return lax.ppermute(value, "c", [(0, 1), (1, 0)])


def exchanged(value):
    return lax.all_to_all(value, PEERS, split_axis=0, concat_axis=0, tiled=True)


def folded(matrices):
    row = lax.broadcasted_iota(jnp.int32, (FOLD_ROWS, FOLD_COLS), 0)
    col = lax.broadcasted_iota(jnp.int32, (FOLD_ROWS, FOLD_COLS), 1)
    plain = jnp.pad(matrices, ((0, 0), (0, 0), (1, 0)))[:, :FOLD_ROWS]
    turned = jnp.pad(matrices[:, ::-1, ::-1], ((0, 0), (0, 0), (0, 1)))[:, :FOLD_ROWS]
    return jnp.where(col <= row, turned, plain).reshape(-1, FOLD)


def shards(init_state, torque, contact, mass_inverse, *vectors):
    core = lax.axis_index("c").astype(jnp.int32)
    chip = (lax.axis_index("x") * lax.axis_size("z") + lax.axis_index("z")).astype(jnp.int32)

    smem = pl.BlockSpec(memory_space=pltpu.SMEM)
    hbm = pl.BlockSpec(memory_space=pltpu.HBM)
    vmem = pl.BlockSpec(memory_space=pltpu.VMEM)
    steps, dof = torque.shape[:2]
    shapes = [(8, 4, LANES), (PAD, 8), (dof, 2, dof), SWAP, SWAP]
    counts, par, mass, own, send = pl.pallas_call(
        split_kernel,
        in_specs=[smem] + [hbm] * 8,
        out_specs=(vmem,) * len(shapes),
        out_shape=tuple(jax.ShapeDtypeStruct(shape, f32) for shape in shapes),
        scratch_shapes=[
            pltpu.VMEM((steps, 2 * LANES), jnp.int32),
            pltpu.VMEM((dof, steps, 2 * LANES), f32),
            pltpu.VMEM((5, 1, dof), f32),
            pltpu.VMEM((LANES, LANES), f32),
            pltpu.SemaphoreType.DMA((8,)),
        ],
        compiler_params=pltpu.CompilerParams(vmem_limit_bytes=ALL_VMEM),
        name="split",
    )(
        core[None],
        contact,
        torque.transpose(1, 0, 2),
        mass_inverse.transpose(1, 0, 2),
        *[v[None] for v in vectors],
    )
    back = swapped(send)
    counts = lax.all_to_all(counts, ("c", "y"), split_axis=0, concat_axis=0, tiled=True)
    totals = counts.reshape(2, BLOCKS, 4, LANES).sum(axis=1).reshape(8, LANES)
    order = core == 0
    mass_back = swapped(mass)
    matrices = folded(
        jnp.where(
            order,
            jnp.concatenate([mass, mass_back], axis=1),
            jnp.concatenate([mass_back, mass], axis=1),
        ).transpose(1, 0, 2)
    )
    mass_rows = matrices[:, : MASS_ROWS * LANES].reshape(GROUP * MASS_ROWS, LANES)
    mass_tails = matrices[:, MASS_ROWS * LANES :].T

    sent = local_call(
        pack_kernel,
        "pack",
        [(CHIPS, CHUNKS, LANES)],
        [(3 * LANES, LANES)],
        core[None],
        own,
        back,
        totals,
        mass_rows,
        mass_tails,
    )
    sent, place, par, init = lax.optimization_barrier(
        (sent, jnp.stack([chip, core]), par, init_state)
    )
    solved = main_call(place, init, exchanged(sent), par)
    mine, send = local_call(
        unpack_kernel, "unpack", [SWAP, SWAP], [(3 * LANES, LANES)], core[None], exchanged(solved)
    )
    final, corr = local_call(
        join_kernel, "join", [(2 * DOF, 2, 2 * LANES), (ITERS, 2 * LANES)], [], core[None], mine, swapped(send)
    )
    return final.transpose(1, 0, 2), corr


def solution(mesh):
    torus = Mesh(mesh.devices.reshape(4, 8, 2, mesh.shape["env"]), ("x", "z", "c", "y"))
    return jax.shard_map(
        shards,
        mesh=torus,
        in_specs=(P(None, "y"), P(TM, None, "y"), P(TM, "y"), P(TM, None, None), P(), P(), P(), P(), P()),
        out_specs=(P(TM, None, "y"), P(None, "y")),
        check_vma=False,
    )
```

```python
import functools
import math

import jax
import jax.numpy as jnp
from jax import lax
from jax.experimental import pallas as pl
from jax.experimental.pallas import tpu as pltpu
from jax.sharding import Mesh
from jax.sharding import PartitionSpec as P

DOF = 35
PAD = 40
HS = 2
SUB = 32
ITERS = 3
GROUP = 4
BLOCKS = 4
CHIPS = 32
STEPS = GROUP * HS
LANES = 128
ENV = 1024
MAIN = 32
DENSE = BLOCKS * MAIN + 16
STATE = 2 * DOF
ROWS = 72
TM = ("x", "z", "c")
PEERS = ("x", "z")

DT = 0.05
FINE = DT / SUB
TURN = 1.0 / (2.0 * math.pi)
SINE = tuple(4.0 * c for c in (6.283182595389212, -16.20867027746649, 16.7609745050196, -9.530799181282873, 3.0583252710952205))

ROW_CONTACT = STEPS * PAD
ROW_COUNT = ROW_CONTACT + 8
ROW_TAIL = ROW_COUNT + 8
IN_ROWS = 12
FOLD_ROWS = 18
FOLD_COLS = 36
FOLD = FOLD_ROWS * FOLD_COLS
MASS_ROWS = 5
CHUNKS = IN_ROWS + GROUP * MASS_ROWS
VMEM_LIMIT = 24 * 1024 * 1024
ALL_VMEM = 67_043_328

f32 = jnp.float32


def lane_index(rows):
    return lax.broadcasted_iota(jnp.int32, (rows, LANES), 1)


def block_transpose(parts):
    lane = lane_index(parts[0].shape[0])
    low = lane < 64
    even = ((lane >> 5) & 1) == 0
    a, b, c, d = parts
    a, c = jnp.where(low, a, pltpu.roll(c, 64, 1)), jnp.where(low, pltpu.roll(a, 64, 1), c)
    b, d = jnp.where(low, b, pltpu.roll(d, 64, 1)), jnp.where(low, pltpu.roll(b, 64, 1), d)
    a, b = jnp.where(even, a, pltpu.roll(b, 32, 1)), jnp.where(even, pltpu.roll(a, 96, 1), b)
    c, d = jnp.where(even, c, pltpu.roll(d, 32, 1)), jnp.where(even, pltpu.roll(c, 96, 1), d)
    return a, b, c, d


def block_spread(value):
    block = lane_index(value.shape[0]) >> 5
    turned = [value] + [pltpu.roll(value, 32 * m, 1) for m in (1, 2, 3)]
    return [
        jnp.where(
            block < 2,
            jnp.where(block == 0, turned[(0 - c) % 4], turned[(1 - c) % 4]),
            jnp.where(block == 2, turned[(2 - c) % 4], turned[(3 - c) % 4]),
        )
        for c in range(4)
    ]


def fine_row(e, i):
    return e * MAIN + i if i < MAIN else BLOCKS * MAIN + 4 * e + i - MAIN


def put_fine(ref, e, part):
    ref[e * MAIN : (e + 1) * MAIN, :] = part[:MAIN]
    ref[fine_row(e, MAIN) : fine_row(e, MAIN) + DOF - MAIN, :] = part[MAIN:DOF]


def get_fine(ref, e):
    tail = ref[fine_row(e, MAIN) : fine_row(e, MAIN) + DOF - MAIN, :]
    return jnp.concatenate([ref[e * MAIN : (e + 1) * MAIN, :], tail])


def unrolled(first, last, body, state):
    for b in range(first, last):
        state = body(b, state)
    return state


def shifted(value, by):
    group = lane_index(value.shape[0]) & 31
    return jnp.where(group >= by, pltpu.roll(value, by, 1), 0.0)


def fold_index(k, i):
    k, i = min(k, i), max(k, i)
    if k < FOLD_ROWS:
        return k * FOLD_COLS + i + 1
    return (DOF - 1 - k) * FOLD_COLS + DOF - 1 - i


def half_of(which):
    return pl.ds(pl.multiple_of(which * LANES, LANES), LANES)


def split_kernel(
    core, contact, torque, mass, v0, v1, v2, v3, v4,
    counts, table, mass_out, own, send,
    contact_in, torque_in, vectors_in, spare, sems,
):
    vectors = (v0, v1, v2, v3, v4)
    pairs = [(contact, contact_in), (torque, torque_in), (mass, mass_out)]
    pairs += [(v, vectors_in.at[i]) for i, v in enumerate(vectors)]
    copies = [pltpu.make_async_copy(a, b, sems.at[i]) for i, (a, b) in enumerate(pairs)]
    for copy in copies:
        copy.start()
    own[...] = jnp.zeros_like(own)
    send[...] = jnp.zeros_like(send)
    spare[...] = jnp.zeros_like(spare)
    copies[0].wait()
    total = jnp.sum(contact_in[...].astype(f32), axis=1, keepdims=True)
    for peer in range(8):
        counts[peer] = jnp.broadcast_to(total, (4, LANES))
    for copy in copies[3:]:
        copy.wait()
    for i in range(len(vectors)):
        spare[i : i + 1, 0:DOF] = vectors_in[i]
    table[...] = spare[...].T[0:PAD, 0:8]
    copies[2].wait()
    copies[1].wait()
    for ref, which in ((own, core[0]), (send, 1 - core[0])):
        part = half_of(which)
        for t in range(4):
            ref[t * PAD : t * PAD + DOF, :] = torque_in[:, t, part]
        ref[4 * PAD : 4 * PAD + 4, :] = contact_in[:, part].astype(f32)


def pack_kernel(core, own, back, totals, mass, tails, out, rows):
    me = core[0]
    rows[...] = jnp.zeros_like(rows)
    for ref, which in ((own, me), (back, 1 - me)):
        rows[pl.ds(pl.multiple_of(which * 4 * PAD, 8), 4 * PAD), :] = ref[0 : 4 * PAD, :]
    own, other = (ref[4 * PAD : 4 * PAD + 4, :] for ref in (own, back))
    rows[ROW_CONTACT : ROW_CONTACT + 8, :] = jnp.where(
        me == 0, jnp.concatenate([own, other]), jnp.concatenate([other, own])
    )
    rows[ROW_COUNT : ROW_COUNT + 8, :] = totals[...]
    block = lane_index(8) >> 5
    tail = jnp.zeros((8, LANES), f32)
    for b in range(GROUP):
        tail = jnp.where(block == b, tails[:, b : b + 1], tail)
    rows[ROW_TAIL : ROW_TAIL + 8, :] = tail
    for c in range(3):
        turned = rows[c * LANES : (c + 1) * LANES, :].T
        for e in range(BLOCKS):
            out[:, e * 3 + c, :] = turned[e * CHIPS : (e + 1) * CHIPS]
    for m in range(GROUP * MASS_ROWS):
        out[:, IN_ROWS + m, :] = jnp.broadcast_to(mass[m : m + 1, :], (CHIPS, LANES))


def main_kernel(
    chip, init_ref, recv, par, out, rows, fold, mb, ma, mx, wide, cols, tau_b, stiff_b, damp_b, grav, spring, fric, start, end, shift, diff, pos, vel, force, vec, corr
):
    for c in range(3):
        rows[c * LANES : (c + 1) * LANES, :] = jnp.concatenate(
            [recv[:, e * 3 + c, :] for e in range(BLOCKS)]
        ).T
    for m in range(MASS_ROWS):
        fold[m * LANES : (m + 1) * LANES, :] = jnp.concatenate(
            [recv[:, IN_ROWS + b * MASS_ROWS + m, :] for b in range(GROUP)]
        ).T
    fold[MASS_ROWS * LANES : FOLD, :] = rows[ROW_TAIL : ROW_TAIL + 8, :]

    def param(i):
        return jnp.broadcast_to(par[:, i : i + 1], (PAD, LANES))

    stiffness, damping, gravity, contact_stiffness, contact_damping = (param(i) for i in range(5))

    for k in range(DOF):
        for i in range(DOF):
            at = fold_index(k, i)
            mb[k, i : i + 1, :] = fold[at : at + 1, :]
        mb[k, DOF:PAD, :] = jnp.zeros((PAD - DOF, LANES), f32)

    def place_mass(n, carry):
        for k in range(5):
            mx[5 * n + k] = jnp.zeros((8, LANES), f32)
            for half in (0, 4):
                mx[5 * n + k, half : half + DOF - MAIN, :] = mb[5 * n + k, MAIN:DOF, :]
            for b, spread in enumerate(block_spread(mb[5 * n + k])):
                ma[b, 5 * n + k] = spread
        return carry

    lax.fori_loop(0, DOF // 5, place_mass, 0)

    mean = rows[ROW_COUNT : ROW_COUNT + 8, :] / ENV
    for t in range(STEPS):
        here = mean[t : t + 1, :]
        spring[t] = (stiffness + gravity + here * contact_stiffness) * (FINE * DT)
        fric[t] = (damping + here * contact_damping) * DT

    for ref in (tau_b, stiff_b, damp_b, grav, shift, pos, vel):
        ref[...] = jnp.zeros_like(ref)
    for j in range(HS):
        turned = block_transpose([rows[(2 * b + j) * PAD : (2 * b + j + 1) * PAD, :] for b in range(GROUP)])
        touch = block_transpose(
            [rows[ROW_CONTACT + 2 * b + j : ROW_CONTACT + 2 * b + j + 1, :] for b in range(GROUP)]
        )
        for e in range(BLOCKS):
            put_fine(tau_b.at[j], e, turned[e] * (FINE * FINE * TURN))
            put_fine(stiff_b.at[j], e, (stiffness + touch[e] * contact_stiffness) * (FINE * FINE))
            put_fine(damp_b.at[j], e, (damping + touch[e] * contact_damping) * FINE)
            put_fine(grav, e, gravity * (FINE * FINE * TURN))

    def half_step(b, t, states, driven):
        moved = []
        for n, (q, w) in enumerate(states):
            pull = spring[t] * q + fric[t] * w
            if driven:
                pull = rows[pl.ds(pl.multiple_of(t * PAD, 8), PAD), :] * (FINE * DT * TURN) - pull
            else:
                pull = -pull
            vec[n, 0:PAD, :] = pull
            moved.append(w)
        for k in range(DOF):
            mass = ma[b, k]
            for n in range(len(states)):
                moved[n] = moved[n] + mass * vec[n, k : k + 1, :]
        return tuple((q + float(SUB) * w, w) for (q, _), w in zip(states, moved))

    def slice_step(b, states, driven):
        return half_step(b, 2 * b + 1, half_step(b, 2 * b, states, driven), driven)

    def one_slice(b, q, w, driven):
        return slice_step(b, ((q, w),), driven)[0]

    def apply_wide(level, slot):
        low = high = None
        for k in range(STATE):
            row = vec[slot, k : k + 1, :]
            term = wide[level, k, :PAD, :] * row
            low = term if low is None else low + term
            if k < PAD:
                term = wide[level, k, PAD:, :] * row
                high = term if high is None else high + term
        for k in range(PAD, STATE):
            high = high + wide[level, k, PAD:, :] * vec[slot, k : k + 1, :]
        return low, high

    row80 = lax.broadcasted_iota(jnp.int32, (2 * PAD, LANES), 0)
    col_block = lane_index(2 * PAD) >> 5

    def first_half(base, q, w):
        for c in range(4):
            k = base + c
            r = jnp.minimum(jnp.where(k < DOF, k, k - DOF), DOF - 1)
            row = jnp.where(k < DOF, spring[0, pl.ds(r, 1), :], fric[0, pl.ds(r, 1), :])
            w = w - jnp.where(col_block[:PAD] == c, ma[0, r] * row, 0.0)
        return q + float(SUB) * w, w

    def first_columns(pair, carry):
        states = []
        for n in range(2):
            col = 4 * (2 * pair + n) + col_block
            col = jnp.where(col < DOF, col, col + (PAD - DOF))
            unit = jnp.where(row80 == col, 1.0, 0.0)
            states.append(first_half(4 * (2 * pair + n), unit[:PAD], unit[PAD:]))
        states = half_step(0, 1, states, False)
        states = unrolled(1, GROUP, lambda b, now: slice_step(b, now, False), states)
        for n in range(2):
            cols[2 * pair + n, :DOF, :] = states[n][0][:DOF]
            cols[2 * pair + n, DOF:STATE, :] = states[n][1][:DOF]
            cols[2 * pair + n, STATE:, :] = jnp.zeros((ROWS - STATE, LANES), f32)
        return carry

    lax.fori_loop(0, 9, first_columns, 0)

    def spread_columns(level, by):
        def some(n, carry):
            for m in range(3):
                value = cols[3 * n + m]
                for c, spread in enumerate(block_spread(value)):
                    wide[level, 4 * (3 * n + m) + c] = spread
                if by:
                    cols[3 * n + m] = shifted(value, by)
            return carry

        lax.fori_loop(0, 6, some, 0)

    def more_columns(level):
        def two(pair, carry):
            totals = [None] * 4
            for k in range(STATE):
                parts = (wide[level - 1, k, :PAD, :], wide[level - 1, k, PAD:, :])
                for n in range(2):
                    row = cols[2 * pair + n, k : k + 1, :]
                    for h in range(2):
                        term = parts[h] * row
                        totals[2 * n + h] = term if k == 0 else totals[2 * n + h] + term
            for n in range(2):
                cols[2 * pair + n, :PAD, :] = totals[2 * n]
                cols[2 * pair + n, PAD:, :] = totals[2 * n + 1]
            return carry

        lax.fori_loop(0, 9, two, 0)

    spread_columns(0, 1)
    more_columns(1)
    spread_columns(1, 2)
    more_columns(2)
    spread_columns(2, 0)

    def scan_groups(q, w):
        def add_earlier(level, by, slot, state):
            vec[slot, :PAD, :] = shifted(state[0], by)
            vec[slot, PAD:ROWS, :] = shifted(state[1], by)
            low, high = apply_wide(level, slot)
            return state[0] + low, state[1] + high

        diff[:DOF, :] = q[:DOF]
        diff[DOF:STATE, :] = w[:DOF]
        diff[STATE:, :] = jnp.zeros((2 * PAD - STATE, LANES), f32)
        base = diff[:PAD, :], diff[PAD:ROWS, :]
        base = add_earlier(0, 1, 0, base)
        base = add_earlier(1, 2, 1, base)
        diff[:PAD, :], diff[PAD:ROWS, :] = base
        vec[0, :PAD, :] = shifted(base[0], 4)

        def more(n, now):
            vec[0, PAD:ROWS, :] = shifted(now[1], 4)
            low, high = diff[:PAD, :], diff[PAD:ROWS, :]
            for k in range(PAD):
                row = vec[0, k : k + 1, :]
                low = low + wide[2, k, :PAD, :] * row
                high = high + wide[2, k, PAD:, :] * row
            for k in range(PAD, STATE):
                low = low + wide[2, k, :PAD, :] * vec[0, k : k + 1, :]
            vec[0, :PAD, :] = shifted(low, 4)
            for k in range(PAD, STATE):
                high = high + wide[2, k, PAD:, :] * vec[0, k : k + 1, :]
            return low, high

        diff[:PAD, :], diff[PAD:ROWS, :] = lax.fori_loop(0, 7, more, base)
        used = lax.broadcasted_iota(jnp.int32, (PAD, LANES), 0) < DOF
        return jnp.where(used, diff[:PAD, :], 0.0), jnp.where(used, diff[DOF : DOF + PAD, :], 0.0)

    first = (lane_index(2 * PAD) & 31) == 0
    back_by = LANES - chip[0]
    vec[0] = jnp.zeros((2 * PAD, LANES), f32)
    vec[0, 0:DOF, :] = init_ref[:DOF, half_of(chip[1])] * TURN
    vec[0, PAD : PAD + DOF, :] = init_ref[DOF:, half_of(chip[1])] * (FINE * TURN)
    init = jnp.where(first, pltpu.roll(vec[0], back_by, 1), 0.0)

    def driven_slice(b, qw):
        return one_slice(b, qw[0], qw[1], True)

    q, w = lax.fori_loop(0, GROUP, driven_slice, (init[:PAD], init[PAD:]))
    q, w = scan_groups(q, w)
    first = first[:PAD]
    entry = jnp.where(first, init[:PAD], shifted(q, 1)), jnp.where(first, init[PAD:], shifted(w, 1))

    def driven_keep(b, qw):
        start[b, :PAD, :], start[b, PAD:, :] = qw
        qw = one_slice(b, qw[0], qw[1], True)
        end[b, :PAD, :], end[b, PAD:, :] = qw
        return qw

    lax.fori_loop(0, GROUP, driven_keep, entry)

    corr[...] = jnp.zeros_like(corr)
    upper = lax.broadcasted_iota(jnp.int32, (8, LANES), 0) < 4

    def iteration(it, carry):
        for half, ref in ((0, pos), (PAD, vel)):
            for e, part in enumerate(block_transpose([start[b, half : half + DOF, :] for b in range(GROUP)])):
                put_fine(ref, e, part)

        def substep(n, carry):
            for u in range(8):
                substep_one(n * 8 + u)
            return carry

        def substep_one(n):
            j = n // SUB
            for v in range(DENSE // 8):
                at = slice(8 * v, 8 * v + 8)
                p = pos[at, :]
                f = p - jnp.round(p)
                s = f * f
                poly = SINE[4] * s + SINE[3]
                for coef in (SINE[2], SINE[1], SINE[0]):
                    poly = poly * s + coef
                sine = (f * (0.25 - s)) * poly
                pull = tau_b[j, at, :] - stiff_b[j, at, :] * p - damp_b[j, at, :] * vel[at, :] - grav[at, :] * sine
                force[at, :] = pull
            acc = [vel[e * MAIN : (e + 1) * MAIN, :] for e in range(BLOCKS)]
            tail = [vel[BLOCKS * MAIN + 8 * n : BLOCKS * MAIN + 8 * n + 8, :] for n in range(2)]
            for k in range(DOF):
                mass = mb[k, :MAIN, :]
                rest = mx[k]
                row = [force[fine_row(e, k) : fine_row(e, k) + 1, :] for e in range(BLOCKS)]
                for e in range(BLOCKS):
                    acc[e] = acc[e] + mass * row[e]
                for n in range(2):
                    tail[n] = tail[n] + rest * jnp.where(upper, row[2 * n], row[2 * n + 1])
            now = jnp.concatenate(acc + tail)
            vel[...] = now
            pos[...] = pos[...] + now

        lax.fori_loop(0, HS * SUB // 8, substep, 0)
        for half, ref in ((0, pos), (PAD, vel)):
            for b, part in enumerate(block_transpose([get_fine(ref, e) for e in range(BLOCKS)])):
                shift[b, half : half + DOF, :] = part - end[b, half : half + DOF, :]

        def chain(b, qw):
            q, w = one_slice(b, qw[0], qw[1], False)
            return q + shift[b, :PAD, :], w + shift[b, PAD:, :]

        q, w = unrolled(1, GROUP, chain, (shift[0, :PAD, :], shift[0, PAD:, :]))
        q, w = scan_groups(q, w)

        def keep(b, state):
            q, w, largest = state
            start[b, :PAD, :] = start[b, :PAD, :] + q
            start[b, PAD:, :] = start[b, PAD:, :] + w
            q, w = chain(b, (q, w))
            end[b, :PAD, :] = end[b, :PAD, :] + q
            end[b, PAD:, :] = end[b, PAD:, :] + w
            dq = q * (1.0 / TURN)
            dv = w * (1.0 / (TURN * FINE))
            square = jnp.sum(dq * dq + dv * dv, axis=0, keepdims=True)
            return q, w, jnp.maximum(largest, square)

        _, _, largest = unrolled(
            0, GROUP, keep, (shifted(q, 1), shifted(w, 1), jnp.zeros((1, LANES), f32))
        )
        group = lane_index(1) & 31
        for by in (16, 8, 4, 2, 1):
            other = jnp.where(group >= by, pltpu.roll(largest, by, 1), pltpu.roll(largest, LANES - 32 + by, 1))
            largest = jnp.maximum(largest, other)
        corr[pl.ds(it, 1), :] = jnp.sqrt(largest)
        return carry

    lax.fori_loop(0, ITERS, iteration, 0)

    for b in range(GROUP):
        rows[b * 2 * PAD : b * 2 * PAD + PAD, :] = end[b, :PAD, :] * (1.0 / TURN)
        rows[b * 2 * PAD + PAD : (b + 1) * 2 * PAD, :] = end[b, PAD:, :] * (1.0 / (TURN * FINE))
    rows[GROUP * 2 * PAD : GROUP * 2 * PAD + 8, :] = corr[...]
    for c in range(3):
        turned = rows[c * LANES : (c + 1) * LANES, :].T
        for e in range(BLOCKS):
            at = e * 3 + c
            out[:, at // 4, at % 4, :] = turned[e * CHIPS : (e + 1) * CHIPS]


def unpack_kernel(core, recv, mine, send, rows):
    for c in range(3):
        at = [e * 3 + c for e in range(BLOCKS)]
        rows[c * LANES : (c + 1) * LANES, :] = jnp.concatenate([recv[:, i // 4, i % 4, :] for i in at]).T
    corr = rows[GROUP * 2 * PAD : GROUP * 2 * PAD + 8, :]
    for ref, which in ((mine, core[0]), (send, 1 - core[0])):
        ref[0 : 4 * PAD, :] = rows[pl.ds(pl.multiple_of(which * 4 * PAD, 8), 4 * PAD), :]
        ref[4 * PAD :, :] = corr


def join_kernel(core, mine, back, out, corr):
    for ref, which in ((mine, core[0]), (back, 1 - core[0])):
        part = half_of(which)
        for s in range(2):
            out[0:DOF, s, part] = ref[s * 2 * PAD : s * 2 * PAD + DOF, :]
            out[DOF : 2 * DOF, s, part] = ref[s * 2 * PAD + PAD : s * 2 * PAD + PAD + DOF, :]
        corr[:, part] = ref[4 * PAD : 4 * PAD + ITERS, :]


SWAP = (4 * PAD + 8, LANES)


def local_call(kernel, name, out_shapes, scratch, scalars, *arrays):
    smem = pl.BlockSpec(memory_space=pltpu.SMEM)
    vmem = pl.BlockSpec(memory_space=pltpu.VMEM)
    shapes = tuple(jax.ShapeDtypeStruct(shape, f32) for shape in out_shapes)
    return pl.pallas_call(
        kernel,
        in_specs=[smem] + [vmem] * len(arrays),
        out_specs=tuple(vmem for _ in shapes) if len(shapes) > 1 else vmem,
        out_shape=shapes if len(shapes) > 1 else shapes[0],
        scratch_shapes=[pltpu.VMEM(shape, f32) for shape in scratch],
        compiler_params=pltpu.CompilerParams(vmem_limit_bytes=VMEM_LIMIT),
        name=name,
    )(scalars, *arrays)


def main_call(chip, init, recv, par):
    tile = (PAD, LANES)
    scratch = [
        (3 * LANES, LANES),
        (FOLD, LANES),
        (DOF, *tile),
        (GROUP, DOF, *tile),
        (DOF, 8, LANES),
        (3, 72, ROWS, LANES),
        (18, ROWS, LANES),
        (HS, DENSE, LANES),
        (HS, DENSE, LANES),
        (HS, DENSE, LANES),
        (DENSE, LANES),
        (STEPS, *tile),
        (STEPS, *tile),
        (GROUP, 2 * PAD, LANES),
        (GROUP, 2 * PAD, LANES),
        (GROUP, 2 * PAD, LANES),
        (2 * PAD, LANES),
        (DENSE, LANES),
        (DENSE, LANES),
        (DENSE, LANES),
        (2, 2 * PAD, LANES),
        (8, LANES),
    ]
    return local_call(main_kernel, "parareal", [(CHIPS, 3, 4, LANES)], scratch, chip, init, recv, par)


def swapped(value):
    return lax.ppermute(value, "c", [(0, 1), (1, 0)])


def exchanged(value):
    return lax.all_to_all(value, PEERS, split_axis=0, concat_axis=0, tiled=True)


def folded(matrices):
    row = lax.broadcasted_iota(jnp.int32, (FOLD_ROWS, FOLD_COLS), 0)
    col = lax.broadcasted_iota(jnp.int32, (FOLD_ROWS, FOLD_COLS), 1)
    plain = jnp.pad(matrices, ((0, 0), (0, 0), (1, 0)))[:, :FOLD_ROWS]
    turned = jnp.pad(matrices[:, ::-1, ::-1], ((0, 0), (0, 0), (0, 1)))[:, :FOLD_ROWS]
    return jnp.where(col <= row, turned, plain).reshape(-1, FOLD)


def shards(init_state, torque, contact, mass_inverse, *vectors):
    core = lax.axis_index("c").astype(jnp.int32)
    chip = (lax.axis_index("x") * lax.axis_size("z") + lax.axis_index("z")).astype(jnp.int32)

    smem = pl.BlockSpec(memory_space=pltpu.SMEM)
    hbm = pl.BlockSpec(memory_space=pltpu.HBM)
    vmem = pl.BlockSpec(memory_space=pltpu.VMEM)
    steps, dof = torque.shape[:2]
    shapes = [(8, 4, LANES), (PAD, 8), (dof, 2, dof), SWAP, SWAP]
    counts, par, mass, own, send = pl.pallas_call(
        split_kernel,
        in_specs=[smem] + [hbm] * 8,
        out_specs=(vmem,) * len(shapes),
        out_shape=tuple(jax.ShapeDtypeStruct(shape, f32) for shape in shapes),
        scratch_shapes=[
            pltpu.VMEM((steps, 2 * LANES), jnp.int32),
            pltpu.VMEM((dof, steps, 2 * LANES), f32),
            pltpu.VMEM((5, 1, dof), f32),
            pltpu.VMEM((LANES, LANES), f32),
            pltpu.SemaphoreType.DMA((8,)),
        ],
        compiler_params=pltpu.CompilerParams(vmem_limit_bytes=ALL_VMEM),
        name="split",
    )(
        core[None],
        contact,
        torque.transpose(1, 0, 2),
        mass_inverse.transpose(1, 0, 2),
        *[v[None] for v in vectors],
    )
    back = swapped(send)
    counts = lax.all_to_all(counts, ("c", "y"), split_axis=0, concat_axis=0, tiled=True)
    totals = counts.reshape(2, BLOCKS, 4, LANES).sum(axis=1).reshape(8, LANES)
    order = core == 0
    mass_back = swapped(mass)
    matrices = folded(
        jnp.where(
            order,
            jnp.concatenate([mass, mass_back], axis=1),
            jnp.concatenate([mass_back, mass], axis=1),
        ).transpose(1, 0, 2)
    )
    mass_rows = matrices[:, : MASS_ROWS * LANES].reshape(GROUP * MASS_ROWS, LANES)
    mass_tails = matrices[:, MASS_ROWS * LANES :].T

    sent = local_call(
        pack_kernel,
        "pack",
        [(CHIPS, CHUNKS, LANES)],
        [(3 * LANES, LANES)],
        core[None],
        own,
        back,
        totals,
        mass_rows,
        mass_tails,
    )
    sent, place, par, init = lax.optimization_barrier(
        (sent, jnp.stack([chip, core]), par, init_state)
    )
    solved = main_call(place, init, exchanged(sent), par)
    mine, send = local_call(
        unpack_kernel, "unpack", [SWAP, SWAP], [(3 * LANES, LANES)], core[None], exchanged(solved)
    )
    final, corr = local_call(
        join_kernel, "join", [(2 * DOF, 2, 2 * LANES), (ITERS, 2 * LANES)], [], core[None], mine, swapped(send)
    )
    return final.transpose(1, 0, 2), corr


def solution(mesh):
    torus = Mesh(mesh.devices.reshape(4, 8, 2, mesh.shape["env"]), ("x", "z", "c", "y"))
    return jax.shard_map(
        shards,
        mesh=torus,
        in_specs=(P(None, "y"), P(TM, None, "y"), P(TM, "y"), P(TM, None, None), P(), P(), P(), P(), P()),
        out_specs=(P(TM, None, "y"), P(None, "y")),
        check_vma=False,
    )
```

```python
import functools
import math

import jax
import jax.numpy as jnp
from jax import lax
from jax.experimental import pallas as pl
from jax.experimental.pallas import tpu as pltpu
from jax.sharding import Mesh
from jax.sharding import PartitionSpec as P

DOF = 35
PAD = 40
HS = 2
SUB = 32
ITERS = 3
GROUP = 4
BLOCKS = 4
CHIPS = 32
STEPS = GROUP * HS
LANES = 128
ENV = 1024
MAIN = 32
DENSE = BLOCKS * MAIN + 16
STATE = 2 * DOF
ROWS = 72
TM = ("x", "z", "c")
PEERS = ("x", "z")

DT = 0.05
FINE = DT / SUB
TURN = 1.0 / (2.0 * math.pi)
SINE = tuple(4.0 * c for c in (6.283182595389212, -16.20867027746649, 16.7609745050196, -9.530799181282873, 3.0583252710952205))

ROW_CONTACT = STEPS * PAD
ROW_COUNT = ROW_CONTACT + 8
ROW_TAIL = ROW_COUNT + 8
IN_ROWS = 12
FOLD_ROWS = 18
FOLD_COLS = 36
FOLD = FOLD_ROWS * FOLD_COLS
MASS_ROWS = 5
CHUNKS = IN_ROWS + GROUP * MASS_ROWS
VMEM_LIMIT = 24 * 1024 * 1024
ALL_VMEM = 67_043_328

f32 = jnp.float32


def lane_index(rows):
    return lax.broadcasted_iota(jnp.int32, (rows, LANES), 1)


def block_transpose(parts):
    lane = lane_index(parts[0].shape[0])
    low = lane < 64
    even = ((lane >> 5) & 1) == 0
    a, b, c, d = parts
    a, c = jnp.where(low, a, pltpu.roll(c, 64, 1)), jnp.where(low, pltpu.roll(a, 64, 1), c)
    b, d = jnp.where(low, b, pltpu.roll(d, 64, 1)), jnp.where(low, pltpu.roll(b, 64, 1), d)
    a, b = jnp.where(even, a, pltpu.roll(b, 32, 1)), jnp.where(even, pltpu.roll(a, 96, 1), b)
    c, d = jnp.where(even, c, pltpu.roll(d, 32, 1)), jnp.where(even, pltpu.roll(c, 96, 1), d)
    return a, b, c, d


def block_spread(value):
    block = lane_index(value.shape[0]) >> 5
    turned = [value] + [pltpu.roll(value, 32 * m, 1) for m in (1, 2, 3)]
    return [
        jnp.where(
            block < 2,
            jnp.where(block == 0, turned[(0 - c) % 4], turned[(1 - c) % 4]),
            jnp.where(block == 2, turned[(2 - c) % 4], turned[(3 - c) % 4]),
        )
        for c in range(4)
    ]


def fine_row(e, i):
    return e * MAIN + i if i < MAIN else BLOCKS * MAIN + 4 * e + i - MAIN


def put_fine(ref, e, part):
    ref[e * MAIN : (e + 1) * MAIN, :] = part[:MAIN]
    ref[fine_row(e, MAIN) : fine_row(e, MAIN) + DOF - MAIN, :] = part[MAIN:DOF]


def get_fine(ref, e):
    tail = ref[fine_row(e, MAIN) : fine_row(e, MAIN) + DOF - MAIN, :]
    return jnp.concatenate([ref[e * MAIN : (e + 1) * MAIN, :], tail])


def unrolled(first, last, body, state):
    for b in range(first, last):
        state = body(b, state)
    return state


def shifted(value, by):
    group = lane_index(value.shape[0]) & 31
    return jnp.where(group >= by, pltpu.roll(value, by, 1), 0.0)


def fold_index(k, i):
    k, i = min(k, i), max(k, i)
    if k < FOLD_ROWS:
        return k * FOLD_COLS + i + 1
    return (DOF - 1 - k) * FOLD_COLS + DOF - 1 - i


def half_of(which):
    return pl.ds(pl.multiple_of(which * LANES, LANES), LANES)


def split_kernel(
    core, contact, torque, mass, v0, v1, v2, v3, v4,
    counts, table, mass_out, own, send,
    contact_in, torque_in, vectors_in, spare, sems,
):
    vectors = (v0, v1, v2, v3, v4)
    pairs = [(contact, contact_in), (torque, torque_in), (mass, mass_out)]
    pairs += [(v, vectors_in.at[i]) for i, v in enumerate(vectors)]
    copies = [pltpu.make_async_copy(a, b, sems.at[i]) for i, (a, b) in enumerate(pairs)]
    for copy in copies:
        copy.start()
    own[...] = jnp.zeros_like(own)
    send[...] = jnp.zeros_like(send)
    spare[...] = jnp.zeros_like(spare)
    copies[0].wait()
    total = jnp.sum(contact_in[...].astype(f32), axis=1, keepdims=True)
    for peer in range(8):
        counts[peer] = jnp.broadcast_to(total, (4, LANES))
    for copy in copies[3:]:
        copy.wait()
    for i in range(len(vectors)):
        spare[i : i + 1, 0:DOF] = vectors_in[i]
    table[...] = spare[...].T[0:PAD, 0:8]
    copies[2].wait()
    copies[1].wait()
    for ref, which in ((own, core[0]), (send, 1 - core[0])):
        part = half_of(which)
        for t in range(4):
            ref[t * PAD : t * PAD + DOF, :] = torque_in[:, t, part]
        ref[4 * PAD : 4 * PAD + 4, :] = contact_in[:, part].astype(f32)


def pack_kernel(core, own, back, totals, mass, tails, out, rows):
    me = core[0]
    rows[...] = jnp.zeros_like(rows)
    for ref, which in ((own, me), (back, 1 - me)):
        rows[pl.ds(pl.multiple_of(which * 4 * PAD, 8), 4 * PAD), :] = ref[0 : 4 * PAD, :]
    own, other = (ref[4 * PAD : 4 * PAD + 4, :] for ref in (own, back))
    rows[ROW_CONTACT : ROW_CONTACT + 8, :] = jnp.where(
        me == 0, jnp.concatenate([own, other]), jnp.concatenate([other, own])
    )
    rows[ROW_COUNT : ROW_COUNT + 8, :] = totals[...]
    block = lane_index(8) >> 5
    tail = jnp.zeros((8, LANES), f32)
    for b in range(GROUP):
        tail = jnp.where(block == b, tails[:, b : b + 1], tail)
    rows[ROW_TAIL : ROW_TAIL + 8, :] = tail
    for c in range(3):
        turned = rows[c * LANES : (c + 1) * LANES, :].T
        for e in range(BLOCKS):
            out[:, e * 3 + c, :] = turned[e * CHIPS : (e + 1) * CHIPS]
    for m in range(GROUP * MASS_ROWS):
        out[:, IN_ROWS + m, :] = jnp.broadcast_to(mass[m : m + 1, :], (CHIPS, LANES))


def main_kernel(
    chip, init_ref, recv, par, out, rows, fold, mb, ma, mx, wide, cols, tau_b, stiff_b, damp_b, grav, spring, fric, start, end, shift, diff, pos, vel, force, vec, corr
):
    for c in range(3):
        rows[c * LANES : (c + 1) * LANES, :] = jnp.concatenate(
            [recv[:, e * 3 + c, :] for e in range(BLOCKS)]
        ).T
    for m in range(MASS_ROWS):
        fold[m * LANES : (m + 1) * LANES, :] = jnp.concatenate(
            [recv[:, IN_ROWS + b * MASS_ROWS + m, :] for b in range(GROUP)]
        ).T
    fold[MASS_ROWS * LANES : FOLD, :] = rows[ROW_TAIL : ROW_TAIL + 8, :]

    def param(i):
        return jnp.broadcast_to(par[:, i : i + 1], (PAD, LANES))

    stiffness, damping, gravity, contact_stiffness, contact_damping = (param(i) for i in range(5))

    for k in range(DOF):
        for i in range(DOF):
            at = fold_index(k, i)
            mb[k, i : i + 1, :] = fold[at : at + 1, :]
        mb[k, DOF:PAD, :] = jnp.zeros((PAD - DOF, LANES), f32)

    def place_mass(n, carry):
        for k in range(5):
            mx[5 * n + k] = jnp.zeros((8, LANES), f32)
            for half in (0, 4):
                mx[5 * n + k, half : half + DOF - MAIN, :] = mb[5 * n + k, MAIN:DOF, :]
            for b, spread in enumerate(block_spread(mb[5 * n + k])):
                ma[b, 5 * n + k] = spread
        return carry

    lax.fori_loop(0, DOF // 5, place_mass, 0)

    mean = rows[ROW_COUNT : ROW_COUNT + 8, :] / ENV
    for t in range(STEPS):
        here = mean[t : t + 1, :]
        spring[t] = (stiffness + gravity + here * contact_stiffness) * (FINE * DT)
        fric[t] = (damping + here * contact_damping) * DT

    for ref in (tau_b, stiff_b, damp_b, grav, shift, pos, vel):
        ref[...] = jnp.zeros_like(ref)
    for j in range(HS):
        turned = block_transpose([rows[(2 * b + j) * PAD : (2 * b + j + 1) * PAD, :] for b in range(GROUP)])
        touch = block_transpose(
            [rows[ROW_CONTACT + 2 * b + j : ROW_CONTACT + 2 * b + j + 1, :] for b in range(GROUP)]
        )
        for e in range(BLOCKS):
            put_fine(tau_b.at[j], e, turned[e] * (FINE * FINE * TURN))
            put_fine(stiff_b.at[j], e, (stiffness + touch[e] * contact_stiffness) * (FINE * FINE))
            put_fine(damp_b.at[j], e, (damping + touch[e] * contact_damping) * FINE)
            put_fine(grav, e, gravity * (FINE * FINE * TURN))

    def half_step(b, t, states, driven):
        moved = []
        for n, (q, w) in enumerate(states):
            pull = spring[t] * q + fric[t] * w
            if driven:
                pull = rows[pl.ds(pl.multiple_of(t * PAD, 8), PAD), :] * (FINE * DT * TURN) - pull
            else:
                pull = -pull
            vec[n, 0:PAD, :] = pull
            moved.append(w)
        for k in range(DOF):
            mass = ma[b, k]
            for n in range(len(states)):
                moved[n] = moved[n] + mass * vec[n, k : k + 1, :]
        return tuple((q + float(SUB) * w, w) for (q, _), w in zip(states, moved))

    def slice_step(b, states, driven):
        return half_step(b, 2 * b + 1, half_step(b, 2 * b, states, driven), driven)

    def one_slice(b, q, w, driven):
        return slice_step(b, ((q, w),), driven)[0]

    def apply_wide(level, slot):
        low = high = None
        for k in range(STATE):
            row = vec[slot, k : k + 1, :]
            term = wide[level, k, :PAD, :] * row
            low = term if low is None else low + term
            if k < PAD:
                term = wide[level, k, PAD:, :] * row
                high = term if high is None else high + term
        for k in range(PAD, STATE):
            high = high + wide[level, k, PAD:, :] * vec[slot, k : k + 1, :]
        return low, high

    row80 = lax.broadcasted_iota(jnp.int32, (2 * PAD, LANES), 0)
    col_block = lane_index(2 * PAD) >> 5

    def first_half(base, q, w):
        for c in range(4):
            k = base + c
            r = jnp.minimum(jnp.where(k < DOF, k, k - DOF), DOF - 1)
            row = jnp.where(k < DOF, spring[0, pl.ds(r, 1), :], fric[0, pl.ds(r, 1), :])
            w = w - jnp.where(col_block[:PAD] == c, ma[0, r] * row, 0.0)
        return q + float(SUB) * w, w

    def first_columns(pair, carry):
        states = []
        for n in range(2):
            col = 4 * (2 * pair + n) + col_block
            col = jnp.where(col < DOF, col, col + (PAD - DOF))
            unit = jnp.where(row80 == col, 1.0, 0.0)
            states.append(first_half(4 * (2 * pair + n), unit[:PAD], unit[PAD:]))
        states = half_step(0, 1, states, False)
        states = unrolled(1, GROUP, lambda b, now: slice_step(b, now, False), states)
        for n in range(2):
            cols[2 * pair + n, :DOF, :] = states[n][0][:DOF]
            cols[2 * pair + n, DOF:STATE, :] = states[n][1][:DOF]
            cols[2 * pair + n, STATE:, :] = jnp.zeros((ROWS - STATE, LANES), f32)
        return carry

    lax.fori_loop(0, 9, first_columns, 0)

    def spread_columns(level, by):
        def some(n, carry):
            for m in range(3):
                value = cols[3 * n + m]
                for c, spread in enumerate(block_spread(value)):
                    wide[level, 4 * (3 * n + m) + c] = spread
                if by:
                    cols[3 * n + m] = shifted(value, by)
            return carry

        lax.fori_loop(0, 6, some, 0)

    def more_columns(level):
        def two(pair, carry):
            totals = [None] * 4
            for k in range(STATE):
                parts = (wide[level - 1, k, :PAD, :], wide[level - 1, k, PAD:, :])
                for n in range(2):
                    row = cols[2 * pair + n, k : k + 1, :]
                    for h in range(2):
                        term = parts[h] * row
                        totals[2 * n + h] = term if k == 0 else totals[2 * n + h] + term
            for n in range(2):
                cols[2 * pair + n, :PAD, :] = totals[2 * n]
                cols[2 * pair + n, PAD:, :] = totals[2 * n + 1]
            return carry

        lax.fori_loop(0, 9, two, 0)

    spread_columns(0, 1)
    more_columns(1)
    spread_columns(1, 2)
    more_columns(2)
    spread_columns(2, 0)

    def scan_groups(q, w):
        def add_earlier(level, by, slot, state):
            vec[slot, :PAD, :] = shifted(state[0], by)
            vec[slot, PAD:ROWS, :] = shifted(state[1], by)
            low, high = apply_wide(level, slot)
            return state[0] + low, state[1] + high

        diff[:DOF, :] = q[:DOF]
        diff[DOF:STATE, :] = w[:DOF]
        diff[STATE:, :] = jnp.zeros((2 * PAD - STATE, LANES), f32)
        base = diff[:PAD, :], diff[PAD:ROWS, :]
        base = add_earlier(0, 1, 0, base)
        base = add_earlier(1, 2, 1, base)
        diff[:PAD, :], diff[PAD:ROWS, :] = base
        vec[0, :PAD, :] = shifted(base[0], 4)

        def more(n, now):
            vec[0, PAD:ROWS, :] = shifted(now[1], 4)
            low, high = diff[:PAD, :], diff[PAD:ROWS, :]
            for k in range(PAD):
                row = vec[0, k : k + 1, :]
                low = low + wide[2, k, :PAD, :] * row
                high = high + wide[2, k, PAD:, :] * row
            for k in range(PAD, STATE):
                low = low + wide[2, k, :PAD, :] * vec[0, k : k + 1, :]
            vec[0, :PAD, :] = shifted(low, 4)
            for k in range(PAD, STATE):
                high = high + wide[2, k, PAD:, :] * vec[0, k : k + 1, :]
            return low, high

        diff[:PAD, :], diff[PAD:ROWS, :] = lax.fori_loop(0, 7, more, base)
        used = lax.broadcasted_iota(jnp.int32, (PAD, LANES), 0) < DOF
        return jnp.where(used, diff[:PAD, :], 0.0), jnp.where(used, diff[DOF : DOF + PAD, :], 0.0)

    first = (lane_index(2 * PAD) & 31) == 0
    back_by = LANES - chip[0]
    vec[0] = jnp.zeros((2 * PAD, LANES), f32)
    vec[0, 0:DOF, :] = init_ref[:DOF, half_of(chip[1])] * TURN
    vec[0, PAD : PAD + DOF, :] = init_ref[DOF:, half_of(chip[1])] * (FINE * TURN)
    init = jnp.where(first, pltpu.roll(vec[0], back_by, 1), 0.0)

    def driven_slice(b, qw):
        return one_slice(b, qw[0], qw[1], True)

    q, w = lax.fori_loop(0, GROUP, driven_slice, (init[:PAD], init[PAD:]))
    q, w = scan_groups(q, w)
    first = first[:PAD]
    entry = jnp.where(first, init[:PAD], shifted(q, 1)), jnp.where(first, init[PAD:], shifted(w, 1))

    def driven_keep(b, qw):
        start[b, :PAD, :], start[b, PAD:, :] = qw
        qw = one_slice(b, qw[0], qw[1], True)
        end[b, :PAD, :], end[b, PAD:, :] = qw
        return qw

    lax.fori_loop(0, GROUP, driven_keep, entry)

    corr[...] = jnp.zeros_like(corr)
    upper = lax.broadcasted_iota(jnp.int32, (8, LANES), 0) < 4

    def iteration(it, carry):
        for half, ref in ((0, pos), (PAD, vel)):
            for e, part in enumerate(block_transpose([start[b, half : half + DOF, :] for b in range(GROUP)])):
                put_fine(ref, e, part)

        def substep(n, carry):
            for u in range(16):
                substep_one(n * 16 + u)
            return carry

        def substep_one(n):
            j = n // SUB
            for v in range(DENSE // 8):
                at = slice(8 * v, 8 * v + 8)
                p = pos[at, :]
                f = p - jnp.round(p)
                s = f * f
                poly = SINE[4] * s + SINE[3]
                for coef in (SINE[2], SINE[1], SINE[0]):
                    poly = poly * s + coef
                sine = (f * (0.25 - s)) * poly
                pull = tau_b[j, at, :] - stiff_b[j, at, :] * p - damp_b[j, at, :] * vel[at, :] - grav[at, :] * sine
                force[at, :] = pull
            acc = [vel[e * MAIN : (e + 1) * MAIN, :] for e in range(BLOCKS)]
            tail = [vel[BLOCKS * MAIN + 8 * n : BLOCKS * MAIN + 8 * n + 8, :] for n in range(2)]
            for k in range(DOF):
                mass = mb[k, :MAIN, :]
                rest = mx[k]
                row = [force[fine_row(e, k) : fine_row(e, k) + 1, :] for e in range(BLOCKS)]
                for e in range(BLOCKS):
                    acc[e] = acc[e] + mass * row[e]
                for n in range(2):
                    tail[n] = tail[n] + rest * jnp.where(upper, row[2 * n], row[2 * n + 1])
            now = jnp.concatenate(acc + tail)
            vel[...] = now
            pos[...] = pos[...] + now

        lax.fori_loop(0, HS * SUB // 16, substep, 0)
        for half, ref in ((0, pos), (PAD, vel)):
            for b, part in enumerate(block_transpose([get_fine(ref, e) for e in range(BLOCKS)])):
                shift[b, half : half + DOF, :] = part - end[b, half : half + DOF, :]

        def chain(b, qw):
            q, w = one_slice(b, qw[0], qw[1], False)
            return q + shift[b, :PAD, :], w + shift[b, PAD:, :]

        q, w = unrolled(1, GROUP, chain, (shift[0, :PAD, :], shift[0, PAD:, :]))
        q, w = scan_groups(q, w)

        def keep(b, state):
            q, w, largest = state
            start[b, :PAD, :] = start[b, :PAD, :] + q
            start[b, PAD:, :] = start[b, PAD:, :] + w
            q, w = chain(b, (q, w))
            end[b, :PAD, :] = end[b, :PAD, :] + q
            end[b, PAD:, :] = end[b, PAD:, :] + w
            dq = q * (1.0 / TURN)
            dv = w * (1.0 / (TURN * FINE))
            square = jnp.sum(dq * dq + dv * dv, axis=0, keepdims=True)
            return q, w, jnp.maximum(largest, square)

        _, _, largest = unrolled(
            0, GROUP, keep, (shifted(q, 1), shifted(w, 1), jnp.zeros((1, LANES), f32))
        )
        group = lane_index(1) & 31
        for by in (16, 8, 4, 2, 1):
            other = jnp.where(group >= by, pltpu.roll(largest, by, 1), pltpu.roll(largest, LANES - 32 + by, 1))
            largest = jnp.maximum(largest, other)
        corr[pl.ds(it, 1), :] = jnp.sqrt(largest)
        return carry

    lax.fori_loop(0, ITERS, iteration, 0)

    for b in range(GROUP):
        rows[b * 2 * PAD : b * 2 * PAD + PAD, :] = end[b, :PAD, :] * (1.0 / TURN)
        rows[b * 2 * PAD + PAD : (b + 1) * 2 * PAD, :] = end[b, PAD:, :] * (1.0 / (TURN * FINE))
    rows[GROUP * 2 * PAD : GROUP * 2 * PAD + 8, :] = corr[...]
    for c in range(3):
        turned = rows[c * LANES : (c + 1) * LANES, :].T
        for e in range(BLOCKS):
            at = e * 3 + c
            out[:, at // 4, at % 4, :] = turned[e * CHIPS : (e + 1) * CHIPS]


def unpack_kernel(core, recv, mine, send, rows):
    for c in range(3):
        at = [e * 3 + c for e in range(BLOCKS)]
        rows[c * LANES : (c + 1) * LANES, :] = jnp.concatenate([recv[:, i // 4, i % 4, :] for i in at]).T
    corr = rows[GROUP * 2 * PAD : GROUP * 2 * PAD + 8, :]
    for ref, which in ((mine, core[0]), (send, 1 - core[0])):
        ref[0 : 4 * PAD, :] = rows[pl.ds(pl.multiple_of(which * 4 * PAD, 8), 4 * PAD), :]
        ref[4 * PAD :, :] = corr


def join_kernel(core, mine, back, out, corr):
    for ref, which in ((mine, core[0]), (back, 1 - core[0])):
        part = half_of(which)
        for s in range(2):
            out[0:DOF, s, part] = ref[s * 2 * PAD : s * 2 * PAD + DOF, :]
            out[DOF : 2 * DOF, s, part] = ref[s * 2 * PAD + PAD : s * 2 * PAD + PAD + DOF, :]
        corr[:, part] = ref[4 * PAD : 4 * PAD + ITERS, :]


SWAP = (4 * PAD + 8, LANES)


def local_call(kernel, name, out_shapes, scratch, scalars, *arrays):
    smem = pl.BlockSpec(memory_space=pltpu.SMEM)
    vmem = pl.BlockSpec(memory_space=pltpu.VMEM)
    shapes = tuple(jax.ShapeDtypeStruct(shape, f32) for shape in out_shapes)
    return pl.pallas_call(
        kernel,
        in_specs=[smem] + [vmem] * len(arrays),
        out_specs=tuple(vmem for _ in shapes) if len(shapes) > 1 else vmem,
        out_shape=shapes if len(shapes) > 1 else shapes[0],
        scratch_shapes=[pltpu.VMEM(shape, f32) for shape in scratch],
        compiler_params=pltpu.CompilerParams(vmem_limit_bytes=VMEM_LIMIT),
        name=name,
    )(scalars, *arrays)


def main_call(chip, init, recv, par):
    tile = (PAD, LANES)
    scratch = [
        (3 * LANES, LANES),
        (FOLD, LANES),
        (DOF, *tile),
        (GROUP, DOF, *tile),
        (DOF, 8, LANES),
        (3, 72, ROWS, LANES),
        (18, ROWS, LANES),
        (HS, DENSE, LANES),
        (HS, DENSE, LANES),
        (HS, DENSE, LANES),
        (DENSE, LANES),
        (STEPS, *tile),
        (STEPS, *tile),
        (GROUP, 2 * PAD, LANES),
        (GROUP, 2 * PAD, LANES),
        (GROUP, 2 * PAD, LANES),
        (2 * PAD, LANES),
        (DENSE, LANES),
        (DENSE, LANES),
        (DENSE, LANES),
        (2, 2 * PAD, LANES),
        (8, LANES),
    ]
    return local_call(main_kernel, "parareal", [(CHIPS, 3, 4, LANES)], scratch, chip, init, recv, par)


def swapped(value):
    return lax.ppermute(value, "c", [(0, 1), (1, 0)])


def exchanged(value):
    return lax.all_to_all(value, PEERS, split_axis=0, concat_axis=0, tiled=True)


def folded(matrices):
    row = lax.broadcasted_iota(jnp.int32, (FOLD_ROWS, FOLD_COLS), 0)
    col = lax.broadcasted_iota(jnp.int32, (FOLD_ROWS, FOLD_COLS), 1)
    plain = jnp.pad(matrices, ((0, 0), (0, 0), (1, 0)))[:, :FOLD_ROWS]
    turned = jnp.pad(matrices[:, ::-1, ::-1], ((0, 0), (0, 0), (0, 1)))[:, :FOLD_ROWS]
    return jnp.where(col <= row, turned, plain).reshape(-1, FOLD)


def shards(init_state, torque, contact, mass_inverse, *vectors):
    core = lax.axis_index("c").astype(jnp.int32)
    chip = (lax.axis_index("x") * lax.axis_size("z") + lax.axis_index("z")).astype(jnp.int32)

    smem = pl.BlockSpec(memory_space=pltpu.SMEM)
    hbm = pl.BlockSpec(memory_space=pltpu.HBM)
    vmem = pl.BlockSpec(memory_space=pltpu.VMEM)
    steps, dof = torque.shape[:2]
    shapes = [(8, 4, LANES), (PAD, 8), (dof, 2, dof), SWAP, SWAP]
    counts, par, mass, own, send = pl.pallas_call(
        split_kernel,
        in_specs=[smem] + [hbm] * 8,
        out_specs=(vmem,) * len(shapes),
        out_shape=tuple(jax.ShapeDtypeStruct(shape, f32) for shape in shapes),
        scratch_shapes=[
            pltpu.VMEM((steps, 2 * LANES), jnp.int32),
            pltpu.VMEM((dof, steps, 2 * LANES), f32),
            pltpu.VMEM((5, 1, dof), f32),
            pltpu.VMEM((LANES, LANES), f32),
            pltpu.SemaphoreType.DMA((8,)),
        ],
        compiler_params=pltpu.CompilerParams(vmem_limit_bytes=ALL_VMEM),
        name="split",
    )(
        core[None],
        contact,
        torque.transpose(1, 0, 2),
        mass_inverse.transpose(1, 0, 2),
        *[v[None] for v in vectors],
    )
    back = swapped(send)
    counts = lax.all_to_all(counts, ("c", "y"), split_axis=0, concat_axis=0, tiled=True)
    totals = counts.reshape(2, BLOCKS, 4, LANES).sum(axis=1).reshape(8, LANES)
    order = core == 0
    mass_back = swapped(mass)
    matrices = folded(
        jnp.where(
            order,
            jnp.concatenate([mass, mass_back], axis=1),
            jnp.concatenate([mass_back, mass], axis=1),
        ).transpose(1, 0, 2)
    )
    mass_rows = matrices[:, : MASS_ROWS * LANES].reshape(GROUP * MASS_ROWS, LANES)
    mass_tails = matrices[:, MASS_ROWS * LANES :].T

    sent = local_call(
        pack_kernel,
        "pack",
        [(CHIPS, CHUNKS, LANES)],
        [(3 * LANES, LANES)],
        core[None],
        own,
        back,
        totals,
        mass_rows,
        mass_tails,
    )
    sent, place, par, init = lax.optimization_barrier(
        (sent, jnp.stack([chip, core]), par, init_state)
    )
    solved = main_call(place, init, exchanged(sent), par)
    mine, send = local_call(
        unpack_kernel, "unpack", [SWAP, SWAP], [(3 * LANES, LANES)], core[None], exchanged(solved)
    )
    final, corr = local_call(
        join_kernel, "join", [(2 * DOF, 2, 2 * LANES), (ITERS, 2 * LANES)], [], core[None], mine, swapped(send)
    )
    return final.transpose(1, 0, 2), corr


def solution(mesh):
    torus = Mesh(mesh.devices.reshape(4, 8, 2, mesh.shape["env"]), ("x", "z", "c", "y"))
    return jax.shard_map(
        shards,
        mesh=torus,
        in_specs=(P(None, "y"), P(TM, None, "y"), P(TM, "y"), P(TM, None, None), P(), P(), P(), P(), P()),
        out_specs=(P(TM, None, "y"), P(None, "y")),
        check_vma=False,
    )
```
